32 devices in a mesh: grid: 8 (over y, x, core), rows: 4 (over z).
Axes of the slice: x: 2, y: 2, z: 4, core: 2. Of those that a mesh axis runs over, the one named last changes fastest.
Arguments:
- density: bfloat16 [32, 128, 4096], P(None, 'rows', 'grid'), as said below
- basis_values: bfloat16 [16, 16, 128, 512], P('grid', None, 'rows'), may hold values from -0.59765625 to 0.59765625
- grid_points: float32 [16, 3, 512], P('grid'), may hold values from -4 to 4
- grid_weights: float32 [16, 512], P('grid'), may hold values from 0.05 to 1
- screened_blocks: int32 [16, 16], P('grid'), may hold values from 0 to 31, as said below
Outputs:
- exchange: float32 [32, 128, 4096], P(None, 'rows', 'grid')
The draws below stay inside these ranges and needn't reach their ends.
Inputs may be any that keep to these rules, and one draw needn't show every extreme that they name: density is symmetric: density[a, i, b * 128 + j] equals density[b, j, a * 128 + i]. `screened_blocks`: each row holds 16 distinct block numbers.
All inputs are finite; a program needn't handle non-finite values.
Results may differ from the reference program's by a relative error of at most 0.00055.
The reference program's roundings to bfloat16 on the way count: a program that leaves them out, or rounds other values in their place, can miss the bound.
Values may be sent and summed in bfloat16 or wider, within the bound.
A program may use at most 128 MiB of HBM per device.

```python
import math
import jax
import jax.numpy as jnp
from jax import lax

NBF = 4096
BS = 128
SIG = 16
PTS = 512
NBLK = 32
NBATCH = 16


def draw_density(key, part):
    key_off, key_diag = jax.random.split(jax.random.fold_in(key, 11), 2)
    noise = jax.random.normal(key_off, (NBF, NBF), jnp.float32) * (0.6 * (2.0 * NBF) ** (-0.5))
    dens = noise + noise.T
    diagonal = jax.random.uniform(key_diag, (NBF,), jnp.float32, 1.6, 2.6)
    dens = dens + jnp.diag(diagonal)
    return dens.reshape(NBF // BS, BS, NBF).astype(jnp.bfloat16)


def draw_screened_blocks(key, part):
    keys = jax.random.split(jax.random.fold_in(key, 7), NBATCH)
    picks = jax.vmap(lambda one_key: jax.random.permutation(one_key, NBF // BS)[:SIG])(keys)
    return picks.astype(jnp.int32)


def level_of(own_key, shape, cuts, least, largest):
    level = 1.0
    for position, shards_of in cuts:
        draws = jax.random.uniform(jax.random.fold_in(jax.random.fold_in(own_key, 6), position), (shards_of,), jnp.float32, least / len(cuts), largest / len(cuts))
        level = level * jnp.repeat(jnp.exp(draws), shape[position] // shards_of).reshape((-1,) + (1,) * (len(shape) - 1 - position))
    return level


def scatter_about(stream_key, extent, deviation, limit, cuts=(), dtype=jnp.bfloat16):
    values = deviation * jax.random.normal(stream_key, extent, jnp.float32)
    if cuts:
        values = values * level_of(stream_key, extent, cuts, -0.22, 0.18)
    return jnp.clip(values, -limit, limit).astype(dtype)


def setup_inputs(seed: int = 0) -> dict:
    key_of = jax.random.split(jax.random.key(seed), 6)
    return {
        "density": draw_density(jax.random.fold_in(key_of[5], 71), 0),
        "basis_values": scatter_about(key_of[1], (NBATCH, SIG, BS, PTS), 0.1, 0.59765625, ((0, 8), (2, 4))),
        "grid_points": jnp.clip(jax.random.uniform(key_of[2], (NBATCH, 3, PTS), jnp.float32, -4.0, 4.0) * level_of(key_of[2], (NBATCH, 3, PTS), ((0, 8),), -0.4, 0.0), -4.0, 4.0),
        "grid_weights": jnp.clip(jnp.exp(math.log(1.0) - 2.9957323 * jax.random.uniform(key_of[3], (NBATCH, PTS), jnp.float32) ** level_of(key_of[3], (NBATCH, PTS), ((0, 8),), -0.2, 0.2)), 0.05, 1.0),
        "screened_blocks": draw_screened_blocks(jax.random.fold_in(key_of[5], 71), 0),
    }


def reference(density, basis_values, grid_points, grid_weights, screened_blocks):
    dense = density.reshape(NBLK, BS, NBLK, BS)

    def one_batch(totals, items):
        values, places, weights, blocks = items
        chosen = dense[blocks][:, :, blocks, :].reshape(SIG * BS, SIG * BS)
        flat = values.reshape(SIG * BS, PTS)
        fmat = jnp.dot(chosen, flat, preferred_element_type=jnp.float32).astype(jnp.bfloat16)
        intersection = jnp.dot(flat.T, fmat, preferred_element_type=jnp.float32)
        diffs = places[:, :, None] - places[:, None, :]
        kern = 1.0 / jnp.sqrt(lax.optimization_barrier(jnp.sum(diffs * diffs, axis=0)) + 0.5)
        mixed = (weights[:, None] * kern * intersection).astype(jnp.bfloat16)
        potential = (jnp.dot(flat, mixed, preferred_element_type=jnp.float32) * weights[None, :]).astype(jnp.bfloat16)
        block_k = jnp.dot(flat, potential.T, preferred_element_type=jnp.float32).reshape(SIG, BS, SIG, BS)
        totals = totals.at[blocks[:, None], :, blocks[None, :], :].add(block_k.transpose(0, 2, 1, 3))
        return (totals, None)
    start_totals = jnp.zeros((NBLK, BS, NBLK, BS), jnp.float32)
    totals, unused = lax.scan(one_batch, start_totals, (basis_values, grid_points, grid_weights, screened_blocks))
    return totals.reshape(NBLK, BS, NBLK * BS)
```

```python
import functools

import jax
import jax.numpy as jnp
from jax import lax
from jax.experimental import pallas as pl
from jax.experimental.pallas import tpu as pltpu
from jax.sharding import PartitionSpec as P

MESH = pl.DeviceIdType.MESH
F32 = jnp.float32
BF16 = jnp.bfloat16
CORES = 2
GROUP = 128
HALVES = 2
OWNERS = 2
LEVELS = 32767.0
TINY = 2.0 ** -110


def kernel(
    ngrid, nrows, sel_ref, p_ref, x_ref, pts_ref, w_ref, out_ref,
    inv, p_all, x_all, psel, fm_send, fm_all, mixed, xpad, pot, lhs, rhs, acc, pair_send, pair_recv,
    q_send, q_recv, s_send, s_recv,
    p_out, p_pair, p_in, x_up, x_down, x_in, fm_out, fm_in, m_up, m_down, m_in,
    pair_out, pair_in, q_out, q_in, s_out, s_in, o_out,
):
    me = lax.axis_index("grid")
    z = lax.axis_index("rows")
    core = lax.rem(me, CORES)
    chip = me // CORES
    nchip = ngrid // CORES
    square = nchip == 4
    partner = chip * CORES + (CORES - 1 - core)
    nblk, rows, cols = p_ref.shape
    nb, nsig, _, npts = x_ref.shape
    bs = rows * nrows
    bpd = cols // bs
    half = npts // HALVES
    quarter = half // OWNERS
    middle = nrows // 2 - 1
    pcuts = 2 if square else 1

    def toward(k):
        if square:
            return chip + (k % 2) * (1 - 2 * lax.rem(chip, 2)) + (k // 2) * (2 - 4 * (chip // 2))
        return lax.rem(chip + k, nchip)

    def source(k):
        return toward(k) if square else lax.rem(chip + nchip - k, nchip)

    def peer(k):
        return toward(k) * CORES + core

    def origin(k):
        return source(k) * CORES + core

    barrier = pltpu.get_barrier_semaphore()
    for k in range(1, nrows):
        pl.semaphore_signal(barrier, inc=1, device_id=(me, lax.rem(z + k, nrows)), device_id_type=MESH)
    for k in range(1, nchip):
        pl.semaphore_signal(barrier, inc=1, device_id=(peer(k), z), device_id_type=MESH)
    pl.semaphore_signal(barrier, inc=1, device_id=(partner, z), device_id_type=MESH)
    for t in range(bpd):
        p_all[me * bpd + t] = p_ref[:, :, t * bs:(t + 1) * bs]
    pl.semaphore_wait(barrier, nrows - 1 + nchip - 1 + 1)

    def remote(src, dst, send, recv, device):
        return pltpu.make_async_remote_copy(
            src_ref=src, dst_ref=dst, send_sem=send, recv_sem=recv, device_id=device, device_id_type=MESH
        )

    def strip(owner):
        return pl.ds(pl.multiple_of(owner * rows, rows), rows)

    def x_copy(batch, h, owner, step, own=False):
        sems = x_up if step > 0 else x_down
        cut = pl.ds(h * half, half)
        slot = x_all.at[batch, :, strip(owner), cut]
        src = x_ref.at[batch, :, :, cut] if own else slot
        return remote(src, slot, sems.at[batch, h, owner], x_in.at[batch, h, owner], (me, z + step))

    def x_begin(batch, up, down):
        for h in range(HALVES):
            @pl.when(jnp.logical_and(z > 0, down))
            def _():
                x_copy(batch, h, z, -1, True).start()

            @pl.when(jnp.logical_and(z < nrows - 1, up))
            def _():
                x_copy(batch, h, z, 1, True).start()

    def x_next(batch, dist):
        if batch < nb:
            x_begin(batch, z == dist, nrows - 1 - z == dist)

    def x_forward(batch, dist):
        for h in range(HALVES):
            @pl.when(jnp.logical_and(z > 0, z + dist < nrows))
            def _():
                x_copy(batch, h, z + dist, -1).wait_recv()
                x_copy(batch, h, z + dist, -1).start()

            @pl.when(jnp.logical_and(z < nrows - 1, z - dist >= 0))
            def _():
                x_copy(batch, h, z - dist, 1).wait_recv()
                x_copy(batch, h, z - dist, 1).start()

    def x_wait(batch, h):
        for dist in range(1, nrows):
            @pl.when(z == 0)
            def _():
                x_copy(batch, h, dist, 1).wait_recv()

            @pl.when(z == nrows - 1)
            def _():
                x_copy(batch, h, nrows - 1 - dist, -1).wait_recv()

    def p_slot(owner, cut):
        span = nblk // pcuts
        return p_all.at[pl.ds(owner * bpd, bpd), pl.ds(cut * span, span)]

    def p_copy(owner, cut, k, to):
        return remote(p_slot(owner, cut), p_slot(owner, cut), p_out.at[k, cut], p_in.at[owner, cut], (peer(to), z))

    def p_forward(k, cut):
        owner = origin(k) if k else me
        return remote(p_slot(owner, cut), p_slot(owner, cut), p_pair.at[k, cut], p_in.at[owner, cut], (partner, z))

    def p_take(k, cut):
        p_copy(origin(k), cut, k, k).wait_recv()
        p_forward(k, cut).start()

    def p_relay(k, cut):
        return p_copy(origin(k), cut, 3, 3 - k)

    x_begin(0, True, True)
    x_next(1, 0)
    if square:
        for k, cut in ((1, 0), (2, 1), (1, 1), (2, 0)):
            p_copy(me, cut, k, k).start()
    else:
        for k in range(1, nchip):
            p_copy(me, 0, k, k).start()
    for cut in range(pcuts):
        p_forward(0, cut).start()

    for batch in range(nb):
        x_all[batch, :, strip(z), :] = x_ref[batch]
        xpad[batch, 0:nsig] = x_ref[batch]
        xpad[batch, nsig] = jnp.zeros((rows, npts), BF16)
        pot[batch, nsig] = jnp.zeros((bs, npts), BF16)

        def invert(block, carry):
            found = jnp.int32(nsig)
            for s in range(nsig):
                found = jnp.where(sel_ref[batch, s] == block, jnp.int32(s), found)
            inv[batch, block] = found
            return carry
        lax.fori_loop(0, nblk, invert, 0)

        def fill(block, carry):
            lhs[pl.ds(pl.multiple_of(block * rows, rows), rows), batch * npts:(batch + 1) * npts] = xpad[
                batch, inv[batch, block]
            ]
            return carry
        lax.fori_loop(0, nblk, fill, 0)

    def fm_copy(batch, h, o):
        return remote(
            fm_send.at[batch, h, o], fm_all.at[batch, h, :, strip(z), :], fm_out.at[batch, h, o],
            fm_in.at[batch, h, z], (me, middle + o),
        )

    def fm_wait(batch, h, other):
        return remote(
            fm_send.at[batch, h, 0], fm_all.at[batch, h, :, strip(other), :], fm_out.at[batch, h, 0],
            fm_in.at[batch, h, other], (me, other),
        )

    def choose(batch):
        def pick(s, carry):
            for t in range(nsig):
                psel[pl.ds(pl.multiple_of(s * rows, rows), rows), t * bs:(t + 1) * bs] = p_all[
                    sel_ref[batch, t], sel_ref[batch, s]
                ]
            return carry
        lax.fori_loop(0, nsig, pick, 0)

    def products(batch, h):
        got = jnp.dot(
            psel[...], x_all[batch, :, :, h * half:(h + 1) * half].reshape(nsig * bs, half),
            preferred_element_type=F32,
        ).astype(BF16)
        for o in range(OWNERS):
            fm_send[batch, h, o] = got[:, o * quarter:(o + 1) * quarter].reshape(nsig, rows, quarter)
        for o in range(OWNERS):
            @pl.when(z != middle + o)
            def _():
                fm_copy(batch, h, o).start()

            @pl.when(z == middle + o)
            def _():
                fm_all[batch, h, :, strip(z), :] = fm_send[batch, h, o]

    def m_copy(batch, h, o, step):
        sems = m_up if step > 0 else m_down
        piece = mixed.at[batch, h, pl.ds(o * quarter, quarter)]
        return remote(piece, piece, sems.at[batch, h, o], m_in.at[batch, h, o], (me, z + step))

    def mix(batch, h, o):
        @pl.when(z == middle + o)
        def _():
            for other in range(nrows):
                if other != middle + o:
                    fm_wait(batch, h, other).wait_recv()
            at = h * half + o * quarter
            lanes = slice(at, at + quarter)
            flipped = jnp.concatenate(
                [pts_ref[axis, batch:batch + 1, lanes] for axis in range(3)] + [jnp.zeros((5, quarter), F32)], axis=0
            ).T
            inter = lax.dot_general(
                fm_all[batch, h].reshape(nsig * bs, quarter), x_all[batch].reshape(nsig * bs, npts),
                (((0,), (0,)), ((), ())), preferred_element_type=F32,
            )
            dist2 = None
            for axis in range(3):
                diff = flipped[:, axis:axis + 1] - pts_ref[axis, batch:batch + 1, :]
                dist2 = diff * diff if dist2 is None else dist2 + diff * diff
            kern = 1.0 / jnp.sqrt(dist2 + 0.5)
            mixed[batch, h, o * quarter:(o + 1) * quarter, :] = (w_ref[batch:batch + 1, :] * kern * inter).astype(BF16)
            if middle + o > 0:
                m_copy(batch, h, o, -1).start()
            if middle + o < nrows - 1:
                m_copy(batch, h, o, 1).start()

    def m_pass(batch, h):
        for o in range(OWNERS):
            @pl.when(z < middle + o)
            def _():
                m_copy(batch, h, o, -1).wait_recv()

                @pl.when(z > 0)
                def _():
                    m_copy(batch, h, o, -1).start()

            @pl.when(z > middle + o)
            def _():
                m_copy(batch, h, o, 1).wait_recv()

                @pl.when(z < nrows - 1)
                def _():
                    m_copy(batch, h, o, 1).start()

    def potentials(batch, h):
        cut = slice(h * half, (h + 1) * half)

        def fill_pot(i, carry):
            some = pl.ds(i * 4, 4)
            got = lax.dot_general(
                x_all[batch, some].reshape(4 * bs, npts), mixed[batch, h], (((1,), (1,)), ((), ())),
                preferred_element_type=F32,
            ) * w_ref[batch:batch + 1, cut]
            pot[batch, some, :, cut] = got.astype(BF16).reshape(4, bs, half)
            return carry
        lax.fori_loop(0, nsig // 4, fill_pot, 0)

    x_forward(0, 1)
    x_next(1, 1)
    if square:
        for k, cut in ((1, 0), (2, 1)):
            p_take(k, cut)
            p_relay(k, cut).start()
    for dist in range(2, nrows - 1):
        x_forward(0, dist)
        x_next(1, dist)
    if square:
        for k, cut in ((1, 1), (2, 0)):
            p_take(k, cut)
        x_forward(1, 1)
        for cut in range(pcuts):
            p_take(3, cut)
    else:
        x_forward(1, 1)
        for k in range(1, nchip):
            p_take(k, 0)
    for k in range(nchip):
        for cut in range(pcuts):
            slot = source(k) * CORES + (CORES - 1 - core)
            remote(p_slot(slot, cut), p_slot(slot, cut), p_pair.at[k, cut], p_in.at[slot, cut], (partner, z)).wait_recv()
    choose(0)
    for h in range(HALVES):
        x_wait(0, h)
        products(0, h)
    for dist in range(2, nrows - 1):
        x_forward(1, dist)
    choose(1)
    for h in range(HALVES):
        x_wait(1, h)
        products(1, h)
    for h in range(HALVES):
        for o in range(OWNERS):
            mix(0, h, o)
    for h in range(HALVES):
        m_pass(0, h)
    for h in range(HALVES):
        potentials(0, h)
    for h in range(HALVES):
        for o in range(OWNERS):
            mix(1, h, o)
        m_pass(1, h)
    for h in range(HALVES):
        potentials(1, h)

    total_rows = nblk * rows
    side = total_rows // 2
    step_rows = min(2 * GROUP, side)
    steps = total_rows // step_rows
    cut_steps = steps // 2
    groups = step_rows // GROUP

    def fill_rhs(dest):
        for t in range(bpd):
            for batch in range(nb):
                rhs[t * bs:(t + 1) * bs, batch * npts:(batch + 1) * npts] = pot[
                    batch, inv[batch, dest * bpd + t]
                ]

    def span(i):
        return pl.ds(pl.multiple_of(i * step_rows, step_rows), step_rows)

    def product(i):
        return lax.dot_general(lhs[span(i), :], rhs[...], (((1,), (1,)), ((), ())), preferred_element_type=F32)

    def pair_copy(k, i):
        return remote(
            pair_send.at[k, span(i)], pair_recv.at[k, span(i)], pair_out.at[k, i], pair_in.at[k, i], (partner, z)
        )

    def q_copy(k, i, device):
        return remote(q_send.at[k, span(i)], q_recv.at[k, span(i)], q_out.at[k, i], q_in.at[k, i], (device, z))

    def s_copy(k, i, device):
        at = pl.ds(i * groups, groups)
        return remote(s_send.at[k, at], s_recv.at[k, at], s_out.at[k, i], s_in.at[k, i], (device, z))

    def send(k, i, device):
        q_copy(k, i, device).start()
        s_copy(k, i, device).start()

    def arrive(k, i, device):
        q_copy(k, i, device).wait_recv()
        s_copy(k, i, device).wait_recv()

    def out_copy(i):
        return pltpu.make_async_copy(acc.at[span(i)], out_ref.at[span(i)], o_out.at[i])

    def encode(k, i, value):
        for g in range(groups):
            some = value[g * GROUP:(g + 1) * GROUP]
            top = jnp.maximum(jnp.max(jnp.abs(some), axis=0, keepdims=True), TINY)
            group = i * groups + g
            s_send[k, group] = jnp.broadcast_to(top * (1.0 / LEVELS), (8, cols))
            q_send[k, pl.ds(pl.multiple_of(group * GROUP, GROUP), GROUP), :] = (
                jnp.round(some * (LEVELS / top)).astype(jnp.int32).astype(jnp.int16)
            )

    def decode(k, i):
        parts = []
        for g in range(groups):
            group = i * groups + g
            at = pl.ds(pl.multiple_of(group * GROUP, GROUP), GROUP)
            parts.append(q_recv[k, at, :].astype(jnp.int32).astype(F32) * s_recv[k, group, 0:1, :])
        return parts[0] if groups == 1 else jnp.concatenate(parts, axis=0)

    def loop(first, last, step):
        def one(i, carry):
            step(i)
            return carry
        lax.fori_loop(first, last, one, 0)

    def theirs(k):
        fill_rhs(toward(k) * CORES + (CORES - 1 - core))

        def step(i):
            pair_send[k, span(i), :] = product(i)
            pair_copy(k, i).start()
        loop(0, steps, step)

    def ours(k, keeps):
        fill_rhs(toward(k) * CORES + core)
        for first, last, keep in keeps:
            def step(i):
                pair_copy(k, i).wait_recv()
                keep(k, i, product(i) + pair_recv[k, span(i), :])
            loop(first, last, step)

    def keep_code(device):
        def keep(k, i, value):
            encode(k, i, value)
            send(k, i, device)
        return keep

    def keep_value(k, i, value):
        pair_recv[k, span(i), :] = value

    def keep_out(k, i, value):
        acc[span(i), :] = value

    def add(k, first, last, device, final):
        def step(i):
            arrive(k, i, device)
            acc[span(i), :] = acc[span(i), :] + decode(k, i)
            if final:
                out_copy(i).start()
        loop(first, last, step)

    low, high = (0, cut_steps), (cut_steps, steps)
    if square:
        flip = {1: peer(1), 2: peer(2)}
        theirs(3)
        ours(3, [(*low, keep_code(flip[1])), (*high, keep_code(flip[2]))])
        theirs(1)
        theirs(2)
        ours(1, [(*low, keep_code(flip[1])), (*high, keep_value)])
        ours(2, [(*high, keep_code(flip[2])), (*low, keep_value)])
        theirs(0)
        ours(0, [(0, steps, keep_out)])
        for k, cut in ((1, high), (2, low)):
            def relay(i):
                arrive(3, i, flip[3 - k])
                encode(k, i, pair_recv[k, span(i), :] + decode(3, i))
                send(k, i, flip[k])
            loop(*cut, relay)
        add(1, *low, flip[1], False)
        add(2, *high, flip[2], False)
        add(1, *high, flip[1], True)
        add(2, *low, flip[2], True)
        sent = [(3, low, flip[1]), (3, high, flip[2])] + [(k, cut, flip[k]) for k in (1, 2) for cut in (low, high)]
    else:
        for k in range(1, nchip):
            theirs(k)
            ours(k, [(0, steps, keep_code(peer(k)))])
        theirs(0)
        ours(0, [(0, steps, keep_out)])
        for k in range(1, nchip):
            add(k, 0, steps, peer(k), k == nchip - 1)
        sent = [(k, (0, steps), peer(k)) for k in range(1, nchip)]

    for k, cut, device in sent:
        def drain(i):
            q_copy(k, i, device).wait_send()
            s_copy(k, i, device).wait_send()
        loop(*cut, drain)
    for k in range(nchip):
        def drain_pair(i):
            pair_copy(k, i).wait_send()
        loop(0, steps, drain_pair)
        for cut in range(pcuts):
            p_forward(k, cut).wait_send()
            if k > 0:
                p_copy(me, cut, k, k).wait_send()
    for batch in range(nb):
        for h in range(HALVES):
            for o in range(OWNERS):
                @pl.when(z != middle + o)
                def _():
                    fm_copy(batch, h, o).wait_send()

                @pl.when(jnp.logical_and(z > 0, z <= middle + o))
                def _():
                    m_copy(batch, h, o, -1).wait_send()

                @pl.when(jnp.logical_and(z < nrows - 1, z >= middle + o))
                def _():
                    m_copy(batch, h, o, 1).wait_send()
            for owner in range(nrows):
                @pl.when(jnp.logical_and(z > 0, owner >= z))
                def _():
                    x_copy(batch, h, owner, -1).wait_send()

                @pl.when(jnp.logical_and(z < nrows - 1, owner <= z))
                def _():
                    x_copy(batch, h, owner, 1).wait_send()

    def drain_out(i):
        out_copy(i).wait()
    loop(0, steps, drain_out)


def body(ngrid, nrows, density, basis_values, grid_points, grid_weights, screened_blocks):
    nblk, rows, cols = density.shape
    nb, nsig, _, npts = basis_values.shape
    bs = rows * nrows
    nchip = ngrid // CORES
    half = npts // HALVES
    quarter = half // OWNERS
    total_rows = nblk * rows
    steps = total_rows // min(2 * GROUP, total_rows // 2)
    vmem = pl.BlockSpec(memory_space=pltpu.VMEM)
    smem = pl.BlockSpec(memory_space=pltpu.SMEM)
    dma = pltpu.SemaphoreType.DMA
    out = pl.pallas_call(
        functools.partial(kernel, ngrid, nrows),
        out_shape=jax.ShapeDtypeStruct((total_rows, cols), F32),
        in_specs=[smem] + [vmem] * 4,
        out_specs=pl.BlockSpec(memory_space=pl.ANY),
        scratch_shapes=[
            pltpu.SMEM((nb, nblk), jnp.int32),
            pltpu.VMEM((nblk, nblk, rows, bs), BF16),
            pltpu.VMEM((nb, nsig, bs, npts), BF16),
            pltpu.VMEM((nsig * rows, nsig * bs), BF16),
            pltpu.VMEM((nb, HALVES, OWNERS, nsig, rows, quarter), BF16),
            pltpu.VMEM((nb, HALVES, nsig, bs, quarter), BF16),
            pltpu.VMEM((nb, HALVES, half, npts), BF16),
            pltpu.VMEM((nb, nsig + 1, rows, npts), BF16),
            pltpu.VMEM((nb, nsig + 1, bs, npts), BF16),
            pltpu.VMEM((total_rows, nb * npts), BF16),
            pltpu.VMEM((cols, nb * npts), BF16),
            pltpu.VMEM((total_rows, cols), F32),
            pltpu.VMEM((nchip, total_rows, cols), F32),
            pltpu.VMEM((nchip, total_rows, cols), F32),
            pltpu.VMEM((nchip, total_rows, cols), jnp.int16),
            pltpu.VMEM((nchip, total_rows, cols), jnp.int16),
            pltpu.VMEM((nchip, total_rows // GROUP, 8, cols), F32),
            pltpu.VMEM((nchip, total_rows // GROUP, 8, cols), F32),
            dma((nchip, 2)), dma((nchip, 2)), dma((ngrid, 2)),
            dma((nb, HALVES, nrows)), dma((nb, HALVES, nrows)), dma((nb, HALVES, nrows)),
            dma((nb, HALVES, OWNERS)), dma((nb, HALVES, nrows)),
            dma((nb, HALVES, OWNERS)), dma((nb, HALVES, OWNERS)), dma((nb, HALVES, OWNERS)),
            dma((nchip, steps)), dma((nchip, steps)),
            dma((nchip, steps)), dma((nchip, steps)), dma((nchip, steps)), dma((nchip, steps)),
            dma((steps,)),
        ],
        compiler_params=pltpu.CompilerParams(
            collective_id=0, has_side_effects=True, vmem_limit_bytes=63 * 1024 * 1024
        ),
        name="exchange",
    )(screened_blocks, density, basis_values, jnp.transpose(grid_points, (1, 0, 2)), grid_weights)
    return out.reshape(nblk, rows, cols)


def solution(mesh):
    placed = (
        P(None, "rows", "grid"),
        P("grid", None, "rows", None),
        P("grid", None, None),
        P("grid", None),
        P("grid", None),
    )
    return jax.shard_map(
        functools.partial(body, mesh.shape["grid"], mesh.shape["rows"]), mesh=mesh, in_specs=placed,
        out_specs=P(None, "rows", "grid"), check_vma=False,
    )
```

```python
import functools

import jax
import jax.numpy as jnp
from jax import lax
from jax.experimental import pallas as pl
from jax.experimental.pallas import tpu as pltpu
from jax.sharding import PartitionSpec as P

MESH = pl.DeviceIdType.MESH
F32 = jnp.float32
BF16 = jnp.bfloat16
CORES = 2
GROUP = 128
HALVES = 2
OWNERS = 2
LEVELS = 32767.0
TINY = 2.0 ** -110


def kernel(
    ngrid, nrows, sel_hbm, p_hbm, x_hbm, pts_hbm, w_hbm, out_ref,
    sel_ref, pts_ref, w_ref, inv, p_all, x_all, psel, fm_send, fm_all, mixed, xpad, pot, lhs, rhs, acc, pair_send, pair_recv,
    q_send, q_recv, s_send, s_recv,
    p_out, p_pair, p_in, x_up, x_down, x_in, fm_out, fm_in, m_up, m_down, m_in,
    pair_out, pair_in, q_out, q_in, s_out, s_in, o_out, local,
):
    me = lax.axis_index("grid")
    z = lax.axis_index("rows")
    core = lax.rem(me, CORES)
    chip = me // CORES
    nchip = ngrid // CORES
    square = nchip == 4
    partner = chip * CORES + (CORES - 1 - core)
    nblk, rows, cols = p_hbm.shape
    nb, nsig, _, npts = x_hbm.shape
    bs = rows * nrows
    bpd = cols // bs
    half = npts // HALVES
    quarter = half // OWNERS
    middle = nrows // 2 - 1
    pcuts = 2 if square else 1

    def toward(k):
        if square:
            return chip + (k % 2) * (1 - 2 * lax.rem(chip, 2)) + (k // 2) * (2 - 4 * (chip // 2))
        return lax.rem(chip + k, nchip)

    def source(k):
        return toward(k) if square else lax.rem(chip + nchip - k, nchip)

    def peer(k):
        return toward(k) * CORES + core

    def origin(k):
        return source(k) * CORES + core

    barrier = pltpu.get_barrier_semaphore()
    for k in range(1, nrows):
        pl.semaphore_signal(barrier, inc=1, device_id=(me, lax.rem(z + k, nrows)), device_id_type=MESH)
    for k in range(1, nchip):
        pl.semaphore_signal(barrier, inc=1, device_id=(peer(k), z), device_id_type=MESH)
    pl.semaphore_signal(barrier, inc=1, device_id=(partner, z), device_id_type=MESH)

    def strip(owner):
        return pl.ds(pl.multiple_of(owner * rows, rows), rows)

    def fetch(src, dst, at):
        return pltpu.make_async_copy(src, dst, local.at[at])

    x_fetch = [fetch(x_hbm.at[b], x_all.at[b, :, strip(z), :], b) for b in range(nb)]
    p_fetch = [
        fetch(p_hbm.at[:, :, pl.ds(t * bs, bs)], p_all.at[me * bpd + t], nb + t) for t in range(bpd)
    ]
    pad_fetch = [fetch(x_hbm.at[b], xpad.at[b, pl.ds(0, nsig)], nb + bpd + b) for b in range(nb)]
    few_fetch = [
        fetch(src, dst, 2 * nb + bpd + at)
        for at, (src, dst) in enumerate(((sel_hbm, sel_ref), (pts_hbm, pts_ref), (w_hbm, w_ref)))
    ]
    for copy in x_fetch + p_fetch + pad_fetch + few_fetch:
        copy.start()
    pl.semaphore_wait(barrier, nrows - 1 + nchip - 1 + 1)

    def remote(src, dst, send, recv, device):
        return pltpu.make_async_remote_copy(
            src_ref=src, dst_ref=dst, send_sem=send, recv_sem=recv, device_id=device, device_id_type=MESH
        )

    def x_copy(batch, h, owner, step):
        sems = x_up if step > 0 else x_down
        slot = x_all.at[batch, :, strip(owner), pl.ds(h * half, half)]
        return remote(slot, slot, sems.at[batch, h, owner], x_in.at[batch, h, owner], (me, z + step))

    def x_begin(batch, up, down):
        for h in range(HALVES):
            @pl.when(jnp.logical_and(z > 0, down))
            def _():
                x_copy(batch, h, z, -1).start()

            @pl.when(jnp.logical_and(z < nrows - 1, up))
            def _():
                x_copy(batch, h, z, 1).start()

    def x_next(batch, dist):
        if batch < nb:
            x_begin(batch, z == dist, nrows - 1 - z == dist)

    def x_forward(batch, dist):
        for h in range(HALVES):
            @pl.when(jnp.logical_and(z > 0, z + dist < nrows))
            def _():
                x_copy(batch, h, z + dist, -1).wait_recv()
                x_copy(batch, h, z + dist, -1).start()

            @pl.when(jnp.logical_and(z < nrows - 1, z - dist >= 0))
            def _():
                x_copy(batch, h, z - dist, 1).wait_recv()
                x_copy(batch, h, z - dist, 1).start()

    def x_wait(batch, h):
        for dist in range(1, nrows):
            @pl.when(z == 0)
            def _():
                x_copy(batch, h, dist, 1).wait_recv()

            @pl.when(z == nrows - 1)
            def _():
                x_copy(batch, h, nrows - 1 - dist, -1).wait_recv()

    def p_slot(owner, cut):
        span = nblk // pcuts
        return p_all.at[pl.ds(owner * bpd, bpd), pl.ds(cut * span, span)]

    def p_copy(owner, cut, k, to):
        return remote(p_slot(owner, cut), p_slot(owner, cut), p_out.at[k, cut], p_in.at[owner, cut], (peer(to), z))

    def p_forward(k, cut):
        owner = origin(k) if k else me
        return remote(p_slot(owner, cut), p_slot(owner, cut), p_pair.at[k, cut], p_in.at[owner, cut], (partner, z))

    def p_take(k, cut):
        p_copy(origin(k), cut, k, k).wait_recv()
        p_forward(k, cut).start()

    def p_relay(k, cut):
        return p_copy(origin(k), cut, 3, 3 - k)

    for copy in x_fetch:
        copy.wait()
    x_begin(0, True, True)
    x_next(1, 0)
    for copy in p_fetch:
        copy.wait()
    if square:
        for k, cut in ((1, 0), (2, 1), (1, 1), (2, 0)):
            p_copy(me, cut, k, k).start()
    else:
        for k in range(1, nchip):
            p_copy(me, 0, k, k).start()
    for cut in range(pcuts):
        p_forward(0, cut).start()

    for copy in pad_fetch + few_fetch:
        copy.wait()
    for batch in range(nb):
        xpad[batch, nsig] = jnp.zeros((rows, npts), BF16)
        pot[batch, nsig] = jnp.zeros((bs, npts), BF16)

        def invert(block, carry):
            found = jnp.int32(nsig)
            for s in range(nsig):
                found = jnp.where(sel_ref[batch, s] == block, jnp.int32(s), found)
            inv[batch, block] = found
            return carry
        lax.fori_loop(0, nblk, invert, 0)

        def fill(block, carry):
            lhs[pl.ds(pl.multiple_of(block * rows, rows), rows), batch * npts:(batch + 1) * npts] = xpad[
                batch, inv[batch, block]
            ]
            return carry
        lax.fori_loop(0, nblk, fill, 0)

    def fm_copy(batch, h, o):
        return remote(
            fm_send.at[batch, h, o], fm_all.at[batch, h, :, strip(z), :], fm_out.at[batch, h, o],
            fm_in.at[batch, h, z], (me, middle + o),
        )

    def fm_wait(batch, h, other):
        return remote(
            fm_send.at[batch, h, 0], fm_all.at[batch, h, :, strip(other), :], fm_out.at[batch, h, 0],
            fm_in.at[batch, h, other], (me, other),
        )

    def choose(batch):
        def pick(s, carry):
            for t in range(nsig):
                psel[pl.ds(pl.multiple_of(s * rows, rows), rows), t * bs:(t + 1) * bs] = p_all[
                    sel_ref[batch, t], sel_ref[batch, s]
                ]
            return carry
        lax.fori_loop(0, nsig, pick, 0)

    def products(batch, h):
        got = jnp.dot(
            psel[...], x_all[batch, :, :, h * half:(h + 1) * half].reshape(nsig * bs, half),
            preferred_element_type=F32,
        ).astype(BF16)
        for o in range(OWNERS):
            fm_send[batch, h, o] = got[:, o * quarter:(o + 1) * quarter].reshape(nsig, rows, quarter)
        for o in range(OWNERS):
            @pl.when(z != middle + o)
            def _():
                fm_copy(batch, h, o).start()

            @pl.when(z == middle + o)
            def _():
                fm_all[batch, h, :, strip(z), :] = fm_send[batch, h, o]

    def m_copy(batch, h, o, step):
        sems = m_up if step > 0 else m_down
        piece = mixed.at[batch, h, pl.ds(o * quarter, quarter)]
        return remote(piece, piece, sems.at[batch, h, o], m_in.at[batch, h, o], (me, z + step))

    def mix(batch, h, o):
        @pl.when(z == middle + o)
        def _():
            for other in range(nrows):
                if other != middle + o:
                    fm_wait(batch, h, other).wait_recv()
            at = h * half + o * quarter
            lanes = slice(at, at + quarter)
            flipped = jnp.concatenate(
                [pts_ref[axis, batch:batch + 1, lanes] for axis in range(3)] + [jnp.zeros((5, quarter), F32)], axis=0
            ).T
            inter = lax.dot_general(
                fm_all[batch, h].reshape(nsig * bs, quarter), x_all[batch].reshape(nsig * bs, npts),
                (((0,), (0,)), ((), ())), preferred_element_type=F32,
            )
            dist2 = None
            for axis in range(3):
                diff = flipped[:, axis:axis + 1] - pts_ref[axis, batch:batch + 1, :]
                dist2 = diff * diff if dist2 is None else dist2 + diff * diff
            kern = 1.0 / jnp.sqrt(dist2 + 0.5)
            mixed[batch, h, o * quarter:(o + 1) * quarter, :] = (w_ref[batch:batch + 1, :] * kern * inter).astype(BF16)
            if middle + o > 0:
                m_copy(batch, h, o, -1).start()
            if middle + o < nrows - 1:
                m_copy(batch, h, o, 1).start()

    def m_pass(batch, h):
        for o in range(OWNERS):
            @pl.when(z < middle + o)
            def _():
                m_copy(batch, h, o, -1).wait_recv()

                @pl.when(z > 0)
                def _():
                    m_copy(batch, h, o, -1).start()

            @pl.when(z > middle + o)
            def _():
                m_copy(batch, h, o, 1).wait_recv()

                @pl.when(z < nrows - 1)
                def _():
                    m_copy(batch, h, o, 1).start()

    def potentials(batch, h):
        cut = slice(h * half, (h + 1) * half)

        def fill_pot(i, carry):
            some = pl.ds(i * 4, 4)
            got = lax.dot_general(
                x_all[batch, some].reshape(4 * bs, npts), mixed[batch, h], (((1,), (1,)), ((), ())),
                preferred_element_type=F32,
            ) * w_ref[batch:batch + 1, cut]
            pot[batch, some, :, cut] = got.astype(BF16).reshape(4, bs, half)
            return carry
        lax.fori_loop(0, nsig // 4, fill_pot, 0)

    x_forward(0, 1)
    x_next(1, 1)
    if square:
        for k, cut in ((1, 0), (2, 1)):
            p_take(k, cut)
            p_relay(k, cut).start()
    for dist in range(2, nrows - 1):
        x_forward(0, dist)
        x_next(1, dist)
    if square:
        for k, cut in ((1, 1), (2, 0)):
            p_take(k, cut)
        x_forward(1, 1)
        for cut in range(pcuts):
            p_take(3, cut)
    else:
        x_forward(1, 1)
        for k in range(1, nchip):
            p_take(k, 0)
    for k in range(nchip):
        for cut in range(pcuts):
            slot = source(k) * CORES + (CORES - 1 - core)
            remote(p_slot(slot, cut), p_slot(slot, cut), p_pair.at[k, cut], p_in.at[slot, cut], (partner, z)).wait_recv()
    choose(0)
    for h in range(HALVES):
        x_wait(0, h)
        products(0, h)
    for dist in range(2, nrows - 1):
        x_forward(1, dist)
    choose(1)
    for h in range(HALVES):
        x_wait(1, h)
        products(1, h)
    for h in range(HALVES):
        for o in range(OWNERS):
            mix(0, h, o)
    for h in range(HALVES):
        m_pass(0, h)
    for h in range(HALVES):
        potentials(0, h)
    owns = jnp.logical_and(z >= middle, z < middle + OWNERS)
    for h in range(HALVES):
        for o in range(OWNERS):
            mix(1, h, o)
        m_pass(1, h)
        if h < HALVES - 1:
            @pl.when(jnp.logical_not(owns))
            def _():
                potentials(1, h)

    @pl.when(owns)
    def _():
        for h in range(HALVES - 1):
            potentials(1, h)
    potentials(1, HALVES - 1)

    total_rows = nblk * rows
    side = total_rows // 2
    step_rows = min(2 * GROUP, side)
    steps = total_rows // step_rows
    cut_steps = steps // 2
    groups = step_rows // GROUP

    def fill_rhs(dest):
        for t in range(bpd):
            for batch in range(nb):
                rhs[t * bs:(t + 1) * bs, batch * npts:(batch + 1) * npts] = pot[
                    batch, inv[batch, dest * bpd + t]
                ]

    def span(i):
        return pl.ds(pl.multiple_of(i * step_rows, step_rows), step_rows)

    def product(i):
        return lax.dot_general(lhs[span(i), :], rhs[...], (((1,), (1,)), ((), ())), preferred_element_type=F32)

    def pair_copy(k, i):
        return remote(
            pair_send.at[k, span(i)], pair_recv.at[k, span(i)], pair_out.at[k, i], pair_in.at[k, i], (partner, z)
        )

    def q_copy(k, i, device):
        return remote(q_send.at[k, span(i)], q_recv.at[k, span(i)], q_out.at[k, i], q_in.at[k, i], (device, z))

    def s_copy(k, i, device):
        return remote(s_send.at[k, i], s_recv.at[k, i], s_out.at[k, i], s_in.at[k, i], (device, z))

    def send(k, i, device):
        q_copy(k, i, device).start()
        s_copy(k, i, device).start()

    def arrive(k, i, device):
        q_copy(k, i, device).wait_recv()
        s_copy(k, i, device).wait_recv()

    def out_copy(i):
        return pltpu.make_async_copy(acc.at[span(i)], out_ref.at[span(i)], o_out.at[i])

    def encode(k, i, value):
        for g in range(groups):
            some = value[g * GROUP:(g + 1) * GROUP]
            top = jnp.maximum(jnp.max(jnp.abs(some), axis=0, keepdims=True), TINY)
            group = i * groups + g
            s_send[k, i, g:g + 1, :] = top * (1.0 / LEVELS)
            q_send[k, pl.ds(pl.multiple_of(group * GROUP, GROUP), GROUP), :] = (
                jnp.round(some * (LEVELS / top)).astype(jnp.int32).astype(jnp.int16)
            )

    def decode(k, i):
        parts = []
        for g in range(groups):
            group = i * groups + g
            at = pl.ds(pl.multiple_of(group * GROUP, GROUP), GROUP)
            parts.append(q_recv[k, at, :].astype(jnp.int32).astype(F32) * s_recv[k, i, g:g + 1, :])
        return parts[0] if groups == 1 else jnp.concatenate(parts, axis=0)

    def loop(first, last, step):
        def one(i, carry):
            step(i)
            return carry
        lax.fori_loop(first, last, one, 0)

    def theirs(k):
        fill_rhs(toward(k) * CORES + (CORES - 1 - core))

        def step(i):
            pair_send[k, span(i), :] = product(i)
            pair_copy(k, i).start()
        loop(0, steps, step)

    def ours(k, keeps):
        fill_rhs(toward(k) * CORES + core)
        for first, last, keep in keeps:
            def step(i):
                pair_copy(k, i).wait_recv()
                keep(k, i, product(i) + pair_recv[k, span(i), :])
            loop(first, last, step)

    def keep_code(device):
        def keep(k, i, value):
            encode(k, i, value)
            send(k, i, device)
        return keep

    def keep_value(k, i, value):
        pair_recv[k, span(i), :] = value

    def keep_out(k, i, value):
        acc[span(i), :] = value

    def add(k, first, last, device, final):
        def step(i):
            arrive(k, i, device)
            acc[span(i), :] = acc[span(i), :] + decode(k, i)
            if final:
                out_copy(i).start()
        loop(first, last, step)

    low, high = (0, cut_steps), (cut_steps, steps)
    if square:
        flip = {1: peer(1), 2: peer(2)}
        theirs(3)
        ours(3, [(*low, keep_code(flip[1])), (*high, keep_code(flip[2]))])
        theirs(1)
        theirs(2)
        ours(1, [(*low, keep_code(flip[1])), (*high, keep_value)])
        ours(2, [(*high, keep_code(flip[2])), (*low, keep_value)])
        theirs(0)
        ours(0, [(0, steps, keep_out)])
        for k, cut in ((1, high), (2, low)):
            def relay(i):
                arrive(3, i, flip[3 - k])
                encode(k, i, pair_recv[k, span(i), :] + decode(3, i))
                send(k, i, flip[k])
            loop(*cut, relay)
        add(1, *low, flip[1], False)
        add(2, *high, flip[2], False)
        add(1, *high, flip[1], True)
        add(2, *low, flip[2], True)
        sent = [(3, low, flip[1]), (3, high, flip[2])] + [(k, cut, flip[k]) for k in (1, 2) for cut in (low, high)]
    else:
        for k in range(1, nchip):
            theirs(k)
            ours(k, [(0, steps, keep_code(peer(k)))])
        theirs(0)
        ours(0, [(0, steps, keep_out)])
        for k in range(1, nchip):
            add(k, 0, steps, peer(k), k == nchip - 1)
        sent = [(k, (0, steps), peer(k)) for k in range(1, nchip)]

    for k, cut, device in sent:
        def drain(i):
            q_copy(k, i, device).wait_send()
            s_copy(k, i, device).wait_send()
        loop(*cut, drain)
    for k in range(nchip):
        def drain_pair(i):
            pair_copy(k, i).wait_send()
        loop(0, steps, drain_pair)
        for cut in range(pcuts):
            p_forward(k, cut).wait_send()
            if k > 0:
                p_copy(me, cut, k, k).wait_send()
    for batch in range(nb):
        for h in range(HALVES):
            for o in range(OWNERS):
                @pl.when(z != middle + o)
                def _():
                    fm_copy(batch, h, o).wait_send()

                @pl.when(jnp.logical_and(z > 0, z <= middle + o))
                def _():
                    m_copy(batch, h, o, -1).wait_send()

                @pl.when(jnp.logical_and(z < nrows - 1, z >= middle + o))
                def _():
                    m_copy(batch, h, o, 1).wait_send()
            for owner in range(nrows):
                @pl.when(jnp.logical_and(z > 0, owner >= z))
                def _():
                    x_copy(batch, h, owner, -1).wait_send()

                @pl.when(jnp.logical_and(z < nrows - 1, owner <= z))
                def _():
                    x_copy(batch, h, owner, 1).wait_send()

    def drain_out(i):
        out_copy(i).wait()
    loop(0, steps, drain_out)


def body(ngrid, nrows, density, basis_values, grid_points, grid_weights, screened_blocks):
    nblk, rows, cols = density.shape
    nb, nsig, _, npts = basis_values.shape
    bs = rows * nrows
    nchip = ngrid // CORES
    half = npts // HALVES
    quarter = half // OWNERS
    total_rows = nblk * rows
    step_rows = min(2 * GROUP, total_rows // 2)
    steps = total_rows // step_rows
    anywhere = pl.BlockSpec(memory_space=pl.ANY)
    dma = pltpu.SemaphoreType.DMA
    out = pl.pallas_call(
        functools.partial(kernel, ngrid, nrows),
        out_shape=jax.ShapeDtypeStruct((total_rows, cols), F32),
        in_specs=[anywhere] * 5,
        out_specs=anywhere,
        scratch_shapes=[
            pltpu.SMEM((nb, nsig), jnp.int32),
            pltpu.VMEM((3, nb, npts), F32),
            pltpu.VMEM((nb, npts), F32),
            pltpu.SMEM((nb, nblk), jnp.int32),
            pltpu.VMEM((nblk, nblk, rows, bs), BF16),
            pltpu.VMEM((nb, nsig, bs, npts), BF16),
            pltpu.VMEM((nsig * rows, nsig * bs), BF16),
            pltpu.VMEM((nb, HALVES, OWNERS, nsig, rows, quarter), BF16),
            pltpu.VMEM((nb, HALVES, nsig, bs, quarter), BF16),
            pltpu.VMEM((nb, HALVES, half, npts), BF16),
            pltpu.VMEM((nb, nsig + 1, rows, npts), BF16),
            pltpu.VMEM((nb, nsig + 1, bs, npts), BF16),
            pltpu.VMEM((total_rows, nb * npts), BF16),
            pltpu.VMEM((cols, nb * npts), BF16),
            pltpu.VMEM((total_rows, cols), F32),
            pltpu.VMEM((nchip, total_rows, cols), F32),
            pltpu.VMEM((nchip, total_rows, cols), F32),
            pltpu.VMEM((nchip, total_rows, cols), jnp.int16),
            pltpu.VMEM((nchip, total_rows, cols), jnp.int16),
            pltpu.VMEM((nchip, steps, step_rows // GROUP, cols), F32),
            pltpu.VMEM((nchip, steps, step_rows // GROUP, cols), F32),
            dma((nchip, 2)), dma((nchip, 2)), dma((ngrid, 2)),
            dma((nb, HALVES, nrows)), dma((nb, HALVES, nrows)), dma((nb, HALVES, nrows)),
            dma((nb, HALVES, OWNERS)), dma((nb, HALVES, nrows)),
            dma((nb, HALVES, OWNERS)), dma((nb, HALVES, OWNERS)), dma((nb, HALVES, OWNERS)),
            dma((nchip, steps)), dma((nchip, steps)),
            dma((nchip, steps)), dma((nchip, steps)), dma((nchip, steps)), dma((nchip, steps)),
            dma((steps,)), dma((2 * nb + cols // bs + 3,)),
        ],
        compiler_params=pltpu.CompilerParams(
            collective_id=0, has_side_effects=True, vmem_limit_bytes=63 * 1024 * 1024
        ),
        name="exchange",
    )(screened_blocks, density, basis_values, jnp.transpose(grid_points, (1, 0, 2)), grid_weights)
    return out.reshape(nblk, rows, cols)


def solution(mesh):
    placed = (
        P(None, "rows", "grid"),
        P("grid", None, "rows", None),
        P("grid", None, None),
        P("grid", None),
        P("grid", None),
    )
    return jax.shard_map(
        functools.partial(body, mesh.shape["grid"], mesh.shape["rows"]), mesh=mesh, in_specs=placed,
        out_specs=P(None, "rows", "grid"), check_vma=False,
    )
```

```python
import functools

import jax
import jax.numpy as jnp
from jax import lax
from jax.experimental import pallas as pl
from jax.experimental.pallas import tpu as pltpu
from jax.sharding import PartitionSpec as P

MESH = pl.DeviceIdType.MESH
F32 = jnp.float32
BF16 = jnp.bfloat16
CORES = 2
GROUP = 128
HALVES = 2
OWNERS = 2
CHUNKS = 8
LEVELS = 32767.0
TINY = 2.0 ** -110


def kernel(
    ngrid, nrows, sel_hbm, p_hbm, x_hbm, pts_hbm, w_hbm, out_ref,
    sel_ref, pts_ref, w_ref, inv, p_all, x_all, psel, fm_send, fm_all, mixed, xpad, pot, lhs, rhs, acc, pair_send, pair_recv,
    q_send, q_recv, s_send, s_recv,
    p_out, p_pair, p_in, x_up, x_down, x_in, fm_out, fm_in, m_up, m_down, m_in,
    pair_out, pair_in, q_out, q_in, s_out, s_in, o_out, local,
):
    me = lax.axis_index("grid")
    z = lax.axis_index("rows")
    core = lax.rem(me, CORES)
    chip = me // CORES
    nchip = ngrid // CORES
    square = nchip == 4
    partner = chip * CORES + (CORES - 1 - core)
    nblk, rows, cols = p_hbm.shape
    nb, nsig, _, npts = x_hbm.shape
    bs = rows * nrows
    bpd = cols // bs
    half = npts // HALVES
    quarter = half // OWNERS
    middle = nrows // 2 - 1
    owns = jnp.logical_and(z >= middle, z < middle + OWNERS)
    pcuts = 2 if square else 1

    def toward(k):
        if square:
            return chip + (k % 2) * (1 - 2 * lax.rem(chip, 2)) + (k // 2) * (2 - 4 * (chip // 2))
        return lax.rem(chip + k, nchip)

    def source(k):
        return toward(k) if square else lax.rem(chip + nchip - k, nchip)

    def peer(k):
        return toward(k) * CORES + core

    def origin(k):
        return source(k) * CORES + core

    barrier = pltpu.get_barrier_semaphore()
    greeted = jnp.int32(1)
    for other in range(nrows):
        near = jnp.logical_or(other == z + 1, other == z - 1)
        if middle <= other < middle + OWNERS:
            near = other != z
        else:
            near = jnp.logical_or(near, jnp.logical_and(owns, other != z))
        greeted = greeted + near.astype(jnp.int32)

        @pl.when(near)
        def _():
            pl.semaphore_signal(barrier, inc=1, device_id=(me, other), device_id_type=MESH)
    for k in (1, 2) if square else range(1, nchip):
        greeted = greeted + 1
        pl.semaphore_signal(barrier, inc=1, device_id=(peer(k), z), device_id_type=MESH)
    pl.semaphore_signal(barrier, inc=1, device_id=(partner, z), device_id_type=MESH)

    def strip(owner):
        return pl.ds(pl.multiple_of(owner * rows, rows), rows)

    def fetch(src, dst, at):
        return pltpu.make_async_copy(src, dst, local.at[at])

    x_fetch = [fetch(x_hbm.at[b], x_all.at[b, pl.ds(0, nsig), strip(z), :], b) for b in range(nb)]
    p_fetch = [
        fetch(p_hbm.at[:, :, pl.ds(t * bs, bs)], p_all.at[me * bpd + t], nb + t) for t in range(bpd)
    ]
    pad_fetch = [fetch(x_hbm.at[b], xpad.at[b, pl.ds(0, nsig)], nb + bpd + b) for b in range(nb)]
    few_fetch = [
        fetch(src, dst, 2 * nb + bpd + at)
        for at, (src, dst) in enumerate(((sel_hbm, sel_ref), (pts_hbm, pts_ref), (w_hbm, w_ref)))
    ]
    for copy in x_fetch + p_fetch + pad_fetch + few_fetch:
        copy.start()
    pl.semaphore_wait(barrier, greeted)

    def remote(src, dst, send, recv, device):
        return pltpu.make_async_remote_copy(
            src_ref=src, dst_ref=dst, send_sem=send, recv_sem=recv, device_id=device, device_id_type=MESH
        )

    def x_copy(batch, h, owner, step):
        sems = x_up if step > 0 else x_down
        slot = x_all.at[batch, pl.ds(0, nsig), strip(owner), pl.ds(h * half, half)]
        return remote(slot, slot, sems.at[batch, h, owner], x_in.at[batch, h, owner], (me, z + step))

    def x_begin(batch, up, down):
        for h in range(HALVES):
            @pl.when(jnp.logical_and(z > 0, down))
            def _():
                x_copy(batch, h, z, -1).start()

            @pl.when(jnp.logical_and(z < nrows - 1, up))
            def _():
                x_copy(batch, h, z, 1).start()

    def x_next(batch, dist):
        if batch < nb:
            x_begin(batch, z == dist, nrows - 1 - z == dist)

    def x_forward(batch, dist):
        for h in range(HALVES):
            @pl.when(jnp.logical_and(z > 0, z + dist < nrows))
            def _():
                x_copy(batch, h, z + dist, -1).wait_recv()
                x_copy(batch, h, z + dist, -1).start()

            @pl.when(jnp.logical_and(z < nrows - 1, z - dist >= 0))
            def _():
                x_copy(batch, h, z - dist, 1).wait_recv()
                x_copy(batch, h, z - dist, 1).start()

    def x_wait(batch, h):
        for dist in range(1, nrows):
            @pl.when(z == 0)
            def _():
                x_copy(batch, h, dist, 1).wait_recv()

            @pl.when(z == nrows - 1)
            def _():
                x_copy(batch, h, nrows - 1 - dist, -1).wait_recv()

    def p_slot(owner, cut):
        span = nblk // pcuts
        return p_all.at[pl.ds(owner * bpd, bpd), pl.ds(cut * span, span)]

    def p_copy(owner, cut, k, to):
        return remote(p_slot(owner, cut), p_slot(owner, cut), p_out.at[k, cut], p_in.at[owner, cut], (peer(to), z))

    def p_forward(k, cut):
        owner = origin(k) if k else me
        return remote(p_slot(owner, cut), p_slot(owner, cut), p_pair.at[k, cut], p_in.at[owner, cut], (partner, z))

    def p_take(k, cut):
        p_copy(origin(k), cut, k, k).wait_recv()
        p_forward(k, cut).start()

    def p_relay(k, cut):
        return p_copy(origin(k), cut, 3, 3 - k)

    for copy in x_fetch:
        copy.wait()
    x_begin(0, True, True)
    x_next(1, 0)
    for copy in p_fetch:
        copy.wait()
    if square:
        for k, cut in ((1, 0), (2, 1), (1, 1), (2, 0)):
            p_copy(me, cut, k, k).start()
    else:
        for k in range(1, nchip):
            p_copy(me, 0, k, k).start()
    for cut in range(pcuts):
        p_forward(0, cut).start()

    for copy in pad_fetch + few_fetch:
        copy.wait()
    for batch in range(nb):
        x_all[batch, nsig] = jnp.zeros((bs, npts), BF16)
        xpad[batch, nsig] = jnp.zeros((rows, npts), BF16)
        pot[batch, nsig] = jnp.zeros((bs, npts), BF16)

        def invert(block, carry):
            found = jnp.int32(nsig)
            for s in range(nsig):
                found = jnp.where(sel_ref[batch, s] == block, jnp.int32(s), found)
            inv[batch, block] = found
            return carry
        lax.fori_loop(0, nblk, invert, 0)

        def fill(block, carry):
            lhs[pl.ds(pl.multiple_of(block * rows, rows), rows), batch * npts:(batch + 1) * npts] = xpad[
                batch, inv[batch, block]
            ]
            return carry
        lax.fori_loop(0, nblk, fill, 0)

    def fm_copy(batch, h, o):
        return remote(
            fm_send.at[batch, h, o], fm_all.at[batch, h, :, strip(z), :], fm_out.at[batch, h, o],
            fm_in.at[batch, h, z], (me, middle + o),
        )

    def fm_wait(batch, h, other):
        return remote(
            fm_send.at[batch, h, 0], fm_all.at[batch, h, :, strip(other), :], fm_out.at[batch, h, 0],
            fm_in.at[batch, h, other], (me, other),
        )

    def choose(batch):
        def pick(s, carry):
            for t in range(nsig):
                psel[pl.ds(pl.multiple_of(s * rows, rows), rows), t * bs:(t + 1) * bs] = p_all[
                    sel_ref[batch, t], sel_ref[batch, s]
                ]
            return carry
        lax.fori_loop(0, nsig, pick, 0)

    def products(batch, h):
        got = jnp.dot(
            psel[...], x_all[batch, 0:nsig, :, h * half:(h + 1) * half].reshape(nsig * bs, half),
            preferred_element_type=F32,
        ).astype(BF16)
        for o in range(OWNERS):
            fm_send[batch, h, o] = got[:, o * quarter:(o + 1) * quarter].reshape(nsig, rows, quarter)
        for j in range(OWNERS):
            o = jnp.where(z <= middle, OWNERS - 1 - j, j)

            @pl.when(z != middle + o)
            def _():
                fm_copy(batch, h, o).start()
        for o in range(OWNERS):
            @pl.when(z == middle + o)
            def _():
                fm_all[batch, h, :, strip(z), :] = fm_send[batch, h, o]

    def m_copy(batch, h, o, step):
        sems = m_up if step > 0 else m_down
        piece = mixed.at[batch, h, pl.ds(o * quarter, quarter)]
        return remote(piece, piece, sems.at[batch, h, o], m_in.at[batch, h, o], (me, z + step))

    def mix(batch, h, o):
        @pl.when(z == middle + o)
        def _():
            for other in range(nrows):
                if other != middle + o:
                    fm_wait(batch, h, other).wait_recv()
            at = h * half + o * quarter
            lanes = slice(at, at + quarter)
            flipped = jnp.concatenate(
                [pts_ref[axis, batch:batch + 1, lanes] for axis in range(3)] + [jnp.zeros((5, quarter), F32)], axis=0
            ).T
            inter = lax.dot_general(
                fm_all[batch, h].reshape(nsig * bs, quarter), x_all[batch, 0:nsig].reshape(nsig * bs, npts),
                (((0,), (0,)), ((), ())), preferred_element_type=F32,
            )
            dist2 = None
            for axis in range(3):
                diff = flipped[:, axis:axis + 1] - pts_ref[axis, batch:batch + 1, :]
                dist2 = diff * diff if dist2 is None else dist2 + diff * diff
            kern = 1.0 / jnp.sqrt(dist2 + 0.5)
            mixed[batch, h, o * quarter:(o + 1) * quarter, :] = (w_ref[batch:batch + 1, :] * kern * inter).astype(BF16)
            if middle + o > 0:
                m_copy(batch, h, o, -1).start()
            if middle + o < nrows - 1:
                m_copy(batch, h, o, 1).start()

    def m_pass(batch, h):
        for o in range(OWNERS):
            @pl.when(z < middle + o)
            def _():
                m_copy(batch, h, o, -1).wait_recv()

                @pl.when(z > 0)
                def _():
                    m_copy(batch, h, o, -1).start()

            @pl.when(z > middle + o)
            def _():
                m_copy(batch, h, o, 1).wait_recv()

                @pl.when(z < nrows - 1)
                def _():
                    m_copy(batch, h, o, 1).start()

    def potentials(batch, h):
        cut = slice(h * half, (h + 1) * half)

        def fill_pot(i, carry):
            some = pl.ds(i * 4, 4)
            got = lax.dot_general(
                x_all[batch, some].reshape(4 * bs, npts), mixed[batch, h], (((1,), (1,)), ((), ())),
                preferred_element_type=F32,
            ) * w_ref[batch:batch + 1, cut]
            pot[batch, some, :, cut] = got.astype(BF16).reshape(4, bs, half)
            return carry
        lax.fori_loop(0, nsig // 4, fill_pot, 0)

    x_forward(0, 1)
    x_next(1, 1)
    if square:
        for k, cut in ((1, 0), (2, 1)):
            p_take(k, cut)
            p_relay(k, cut).start()
    for dist in range(2, nrows - 1):
        x_forward(0, dist)
        x_next(1, dist)
    if square:
        for k, cut in ((1, 1), (2, 0)):
            p_take(k, cut)
        x_forward(1, 1)
        for cut in range(pcuts):
            p_take(3, cut)
    else:
        x_forward(1, 1)
        for k in range(1, nchip):
            p_take(k, 0)
    for k in range(nchip):
        for cut in range(pcuts):
            slot = source(k) * CORES + (CORES - 1 - core)
            remote(p_slot(slot, cut), p_slot(slot, cut), p_pair.at[k, cut], p_in.at[slot, cut], (partner, z)).wait_recv()
    choose(0)
    for h in range(HALVES):
        x_wait(0, h)
        products(0, h)
    for dist in range(2, nrows - 1):
        x_forward(1, dist)
    choose(1)
    for h in range(HALVES):
        x_wait(1, h)
        products(1, h)
    for h in range(HALVES):
        for o in range(OWNERS):
            mix(0, h, o)
    for h in range(HALVES):
        m_pass(0, h)
    total_rows = nblk * rows
    side = total_rows // 2
    step_rows = min(2 * GROUP, side)
    steps = total_rows // step_rows
    cut_steps = steps // 2
    groups = step_rows // GROUP
    early = (nb - 1) * npts

    def fill_rhs(dest):
        for t in range(bpd):
            for batch in range(nb):
                rhs[t * bs:(t + 1) * bs, batch * npts:(batch + 1) * npts] = pot[
                    batch, inv[batch, dest * bpd + t]
                ]

    def fill_early(dest):
        for t in range(bpd):
            for batch in range(nb - 1):
                rhs[t * bs:(t + 1) * bs, batch * npts:(batch + 1) * npts] = pot[batch, inv[batch, dest * bpd + t]]

    def fill_late(dest):
        batch, known = nb - 1, npts - half
        some = []
        for t in range(bpd):
            slot = inv[batch, dest * bpd + t]
            rhs[t * bs:(t + 1) * bs, early:early + known] = pot[batch, slot, :, 0:known]
            some.append(x_all[batch, slot])
        got = lax.dot_general(
            some[0] if bpd == 1 else jnp.concatenate(some, axis=0), mixed[batch, HALVES - 1],
            (((1,), (1,)), ((), ())), preferred_element_type=F32,
        ) * w_ref[batch:batch + 1, known:npts]
        rhs[:, early + known:nb * npts] = got.astype(BF16)

    def span(i):
        return pl.ds(pl.multiple_of(i * step_rows, step_rows), step_rows)

    def product(i, first=0, last=nb * npts):
        return lax.dot_general(
            lhs[span(i), first:last], rhs[:, first:last], (((1,), (1,)), ((), ())), preferred_element_type=F32
        )

    def pair_copy(k, i):
        return remote(
            pair_send.at[k, span(i)], pair_recv.at[k, span(i)], pair_out.at[k, i], pair_in.at[k, i], (partner, z)
        )

    def q_copy(k, i, device):
        return remote(q_send.at[k, span(i)], q_recv.at[k, span(i)], q_out.at[k, i], q_in.at[k, i], (device, z))

    def s_copy(k, i, device):
        return remote(s_send.at[k, i], s_recv.at[k, i], s_out.at[k, i], s_in.at[k, i], (device, z))

    def send(k, i, device):
        q_copy(k, i, device).start()
        s_copy(k, i, device).start()

    def arrive(k, i, device):
        q_copy(k, i, device).wait_recv()
        s_copy(k, i, device).wait_recv()

    def out_copy(i):
        return pltpu.make_async_copy(acc.at[span(i)], out_ref.at[span(i)], o_out.at[i])

    def encode(k, i, value):
        for g in range(groups):
            some = value[g * GROUP:(g + 1) * GROUP]
            top = jnp.maximum(jnp.max(jnp.abs(some), axis=0, keepdims=True), TINY)
            group = i * groups + g
            s_send[k, i, g:g + 1, :] = top * (1.0 / LEVELS)
            q_send[k, pl.ds(pl.multiple_of(group * GROUP, GROUP), GROUP), :] = (
                jnp.round(some * (LEVELS / top)).astype(jnp.int32).astype(jnp.int16)
            )

    def decode(k, i):
        parts = []
        for g in range(groups):
            group = i * groups + g
            at = pl.ds(pl.multiple_of(group * GROUP, GROUP), GROUP)
            parts.append(q_recv[k, at, :].astype(jnp.int32).astype(F32) * s_recv[k, i, g:g + 1, :])
        return parts[0] if groups == 1 else jnp.concatenate(parts, axis=0)

    def loop(first, last, step):
        def one(i, carry):
            step(i)
            return carry
        lax.fori_loop(first, last, one, 0)

    def theirs(k):
        fill_rhs(toward(k) * CORES + (CORES - 1 - core))

        def step(i):
            pair_send[k, span(i), :] = product(i)
            pair_copy(k, i).start()
        loop(0, steps, step)

    def ours(k, keeps):
        fill_rhs(toward(k) * CORES + core)
        for first, last, keep in keeps:
            def step(i):
                pair_copy(k, i).wait_recv()
                keep(k, i, product(i) + pair_recv[k, span(i), :])
            loop(first, last, step)

    def far_early():
        fill_early(toward(3) * CORES + (CORES - 1 - core))

        def step(i):
            pair_send[3, span(i), :] = product(i, 0, early)
        loop(0, steps, step)
        fill_early(toward(3) * CORES + core)

        def step(i):
            acc[span(i), :] = product(i, 0, early)
        loop(0, steps, step)

    def far_late(device):
        def weave(j):
            return lax.rem(j, 2) * cut_steps + j // 2

        fill_late(toward(3) * CORES + (CORES - 1 - core))

        def step(j):
            i = weave(j)
            pair_send[3, span(i), :] = pair_send[3, span(i), :] + product(i, early)
            pair_copy(3, i).start()
        loop(0, steps, step)
        fill_late(toward(3) * CORES + core)

        def step(j):
            i = weave(j)
            value = acc[span(i), :] + product(i, early)
            pair_copy(3, i).wait_recv()
            encode(3, i, value + pair_recv[3, span(i), :])
            send(3, i, device(i // cut_steps))
        loop(0, steps, step)

    def keep_code(device):
        def keep(k, i, value):
            encode(k, i, value)
            send(k, i, device)
        return keep

    def keep_value(k, i, value):
        pair_recv[k, span(i), :] = value

    def keep_out(k, i, value):
        acc[span(i), :] = value

    def add(k, first, last, device, final):
        def step(i):
            arrive(k, i, device)
            acc[span(i), :] = acc[span(i), :] + decode(k, i)
            if final:
                out_copy(i).start()
        loop(first, last, step)

    def drain(sent):
        for k, cut, device in sent:
            def finish(i):
                q_copy(k, i, device).wait_send()
                s_copy(k, i, device).wait_send()
            loop(*cut, finish)

    def drain_early():
        for k in range(nchip):
            def drain_pair(i):
                pair_copy(k, i).wait_send()
            loop(0, steps, drain_pair)
            for cut in range(pcuts):
                p_forward(k, cut).wait_send()
                if k > 0:
                    p_copy(me, cut, k, k).wait_send()
        for batch in range(nb):
            for h in range(HALVES):
                for o in range(OWNERS):
                    @pl.when(z != middle + o)
                    def _():
                        fm_copy(batch, h, o).wait_send()

                    @pl.when(jnp.logical_and(z > 0, z <= middle + o))
                    def _():
                        m_copy(batch, h, o, -1).wait_send()

                    @pl.when(jnp.logical_and(z < nrows - 1, z >= middle + o))
                    def _():
                        m_copy(batch, h, o, 1).wait_send()
                for owner in range(nrows):
                    @pl.when(jnp.logical_and(z > 0, owner >= z))
                    def _():
                        x_copy(batch, h, owner, -1).wait_send()

                    @pl.when(jnp.logical_and(z < nrows - 1, owner <= z))
                    def _():
                        x_copy(batch, h, owner, 1).wait_send()

    low, high = (0, cut_steps), (cut_steps, steps)
    @pl.when(owns)
    def _():
        for h in range(HALVES):
            for o in range(OWNERS):
                mix(1, h, o)
            if h == 0:
                for other in range(HALVES):
                    potentials(0, other)
        for h in range(HALVES):
            if h == HALVES - 1 and square:
                far_early()
            m_pass(1, h)
        for h in range(HALVES - 1):
            potentials(1, h)

    @pl.when(jnp.logical_not(owns))
    def _():
        for h in range(HALVES):
            potentials(0, h)
        if square:
            far_early()
        for h in range(HALVES):
            m_pass(1, h)
            if h < HALVES - 1:
                potentials(1, h)

    if square:
        flip = {1: peer(1), 2: peer(2)}
        far_late(lambda cut: flip[1] + cut * (flip[2] - flip[1]))
        potentials(1, HALVES - 1)
        theirs(1)
        theirs(2)
        ours(1, [(*low, keep_code(flip[1])), (*high, keep_value)])
        ours(2, [(*high, keep_code(flip[2])), (*low, keep_value)])
        theirs(0)
        ours(0, [(0, steps, keep_out)])
        for k, cut in ((1, high), (2, low)):
            def relay(i):
                arrive(3, i, flip[3 - k])
                encode(k, i, pair_recv[k, span(i), :] + decode(3, i))
                send(k, i, flip[k])
            loop(*cut, relay)
        add(1, *low, flip[1], False)
        add(2, *high, flip[2], False)
        drain([(3, low, flip[1]), (3, high, flip[2]), (1, low, flip[1]), (2, high, flip[2])])
        drain_early()
        add(1, *high, flip[1], True)
        add(2, *low, flip[2], True)
        drain([(1, high, flip[1]), (2, low, flip[2])])
    else:
        potentials(1, HALVES - 1)
        for k in range(1, nchip):
            theirs(k)
            ours(k, [(0, steps, keep_code(peer(k)))])
        theirs(0)
        ours(0, [(0, steps, keep_out)])
        for k in range(1, nchip):
            add(k, 0, steps, peer(k), k == nchip - 1)
        drain([(k, (0, steps), peer(k)) for k in range(1, nchip)])
        drain_early()

    def drain_out(i):
        out_copy(i).wait()
    loop(0, steps, drain_out)


def deliver(sum_ref, out_ref, buf, came, went):
    span = sum_ref.shape[0] // CHUNKS
    cuts = [pl.ds(i * span, span) for i in range(CHUNKS)]
    ins = [pltpu.make_async_copy(sum_ref.at[cut], buf.at[cut], came.at[i]) for i, cut in enumerate(cuts)]
    outs = [pltpu.make_async_copy(buf.at[cut], out_ref.at[cut], went.at[i]) for i, cut in enumerate(cuts)]
    for copy in ins:
        copy.start()
    for copy_in, copy_out in zip(ins, outs):
        copy_in.wait()
        copy_out.start()
    for copy in outs:
        copy.wait()


def body(ngrid, nrows, density, basis_values, grid_points, grid_weights, screened_blocks):
    nblk, rows, cols = density.shape
    nb, nsig, _, npts = basis_values.shape
    bs = rows * nrows
    nchip = ngrid // CORES
    half = npts // HALVES
    quarter = half // OWNERS
    total_rows = nblk * rows
    step_rows = min(2 * GROUP, total_rows // 2)
    steps = total_rows // step_rows
    anywhere = pl.BlockSpec(memory_space=pl.ANY)
    dma = pltpu.SemaphoreType.DMA
    out = pl.pallas_call(
        functools.partial(kernel, ngrid, nrows),
        out_shape=jax.ShapeDtypeStruct((total_rows, cols), F32),
        in_specs=[anywhere] * 5,
        out_specs=anywhere,
        scratch_shapes=[
            pltpu.SMEM((nb, nsig), jnp.int32),
            pltpu.VMEM((3, nb, npts), F32),
            pltpu.VMEM((nb, npts), F32),
            pltpu.SMEM((nb, nblk), jnp.int32),
            pltpu.VMEM((nblk, nblk, rows, bs), BF16),
            pltpu.VMEM((nb, nsig + 1, bs, npts), BF16),
            pltpu.VMEM((nsig * rows, nsig * bs), BF16),
            pltpu.VMEM((nb, HALVES, OWNERS, nsig, rows, quarter), BF16),
            pltpu.VMEM((nb, HALVES, nsig, bs, quarter), BF16),
            pltpu.VMEM((nb, HALVES, half, npts), BF16),
            pltpu.VMEM((nb, nsig + 1, rows, npts), BF16),
            pltpu.VMEM((nb, nsig + 1, bs, npts), BF16),
            pltpu.VMEM((total_rows, nb * npts), BF16),
            pltpu.VMEM((cols, nb * npts), BF16),
            pltpu.VMEM((total_rows, cols), F32),
            pltpu.VMEM((nchip, total_rows, cols), F32),
            pltpu.VMEM((nchip, total_rows, cols), F32),
            pltpu.VMEM((nchip, total_rows, cols), jnp.int16),
            pltpu.VMEM((nchip, total_rows, cols), jnp.int16),
            pltpu.VMEM((nchip, steps, step_rows // GROUP, cols), F32),
            pltpu.VMEM((nchip, steps, step_rows // GROUP, cols), F32),
            dma((nchip, 2)), dma((nchip, 2)), dma((ngrid, 2)),
            dma((nb, HALVES, nrows)), dma((nb, HALVES, nrows)), dma((nb, HALVES, nrows)),
            dma((nb, HALVES, OWNERS)), dma((nb, HALVES, nrows)),
            dma((nb, HALVES, OWNERS)), dma((nb, HALVES, OWNERS)), dma((nb, HALVES, OWNERS)),
            dma((nchip, steps)), dma((nchip, steps)),
            dma((nchip, steps)), dma((nchip, steps)), dma((nchip, steps)), dma((nchip, steps)),
            dma((steps,)), dma((2 * nb + cols // bs + 3,)),
        ],
        compiler_params=pltpu.CompilerParams(
            collective_id=0, has_side_effects=True, vmem_limit_bytes=63 * 1024 * 1024
        ),
        name="exchange",
    )(screened_blocks, density, basis_values, jnp.transpose(grid_points, (1, 0, 2)), grid_weights)
    out = pl.pallas_call(
        deliver,
        out_shape=jax.ShapeDtypeStruct((total_rows, cols), F32),
        in_specs=[anywhere],
        out_specs=anywhere,
        scratch_shapes=[pltpu.VMEM((total_rows, cols), F32), dma((CHUNKS,)), dma((CHUNKS,))],
        name="deliver",
    )(out)
    return out.reshape(nblk, rows, cols)


def solution(mesh):
    placed = (
        P(None, "rows", "grid"),
        P("grid", None, "rows", None),
        P("grid", None, None),
        P("grid", None),
        P("grid", None),
    )
    return jax.shard_map(
        functools.partial(body, mesh.shape["grid"], mesh.shape["rows"]), mesh=mesh, in_specs=placed,
        out_specs=P(None, "rows", "grid"), check_vma=False,
    )
```

```python
import functools

import jax
import jax.numpy as jnp
from jax import lax
from jax.experimental import pallas as pl
from jax.experimental.pallas import tpu as pltpu
from jax.sharding import PartitionSpec as P

MESH = pl.DeviceIdType.MESH
F32 = jnp.float32
BF16 = jnp.bfloat16
CORES = 2
GROUP = 128
HALVES = 2
OWNERS = 2
CHUNKS = 8
LEVELS = 32767.0
TINY = 2.0 ** -110


def kernel(
    ngrid, nrows, sel_hbm, p_hbm, x_hbm, pts_hbm, w_hbm, out_ref,
    sel_ref, pts_ref, w_ref, inv, p_all, x_all, psel, fm_send, fm_all, mixed, xpad, pot, lhs, rhs, acc, pair_send, pair_recv,
    q_send, q_recv, s_send, s_recv,
    p_out, p_pair, p_in, x_up, x_down, x_in, fm_out, fm_in, m_up, m_down, m_in,
    pair_out, pair_in, far_in, q_out, q_in, s_out, s_in, o_out, local,
):
    me = lax.axis_index("grid")
    z = lax.axis_index("rows")
    core = lax.rem(me, CORES)
    chip = me // CORES
    nchip = ngrid // CORES
    square = nchip == 4
    partner = chip * CORES + (CORES - 1 - core)
    nblk, rows, cols = p_hbm.shape
    nb, nsig, _, npts = x_hbm.shape
    bs = rows * nrows
    bpd = cols // bs
    half = npts // HALVES
    quarter = half // OWNERS
    middle = nrows // 2 - 1
    owns = jnp.logical_and(z >= middle, z < middle + OWNERS)
    pcuts = 2 if square else 1

    def toward(k):
        if square:
            return chip + (k % 2) * (1 - 2 * lax.rem(chip, 2)) + (k // 2) * (2 - 4 * (chip // 2))
        return lax.rem(chip + k, nchip)

    def source(k):
        return toward(k) if square else lax.rem(chip + nchip - k, nchip)

    def peer(k):
        return toward(k) * CORES + core

    def origin(k):
        return source(k) * CORES + core

    barrier = pltpu.get_barrier_semaphore()
    greeted = jnp.int32(1)
    for other in range(nrows):
        near = jnp.logical_or(other == z + 1, other == z - 1)
        if middle <= other < middle + OWNERS:
            near = other != z
        else:
            near = jnp.logical_or(near, jnp.logical_and(owns, other != z))
        greeted = greeted + near.astype(jnp.int32)

        @pl.when(near)
        def _():
            pl.semaphore_signal(barrier, inc=1, device_id=(me, other), device_id_type=MESH)
    for k in (1, 2) if square else range(1, nchip):
        greeted = greeted + 1
        pl.semaphore_signal(barrier, inc=1, device_id=(peer(k), z), device_id_type=MESH)
    pl.semaphore_signal(barrier, inc=1, device_id=(partner, z), device_id_type=MESH)

    def strip(owner):
        return pl.ds(pl.multiple_of(owner * rows, rows), rows)

    def fetch(src, dst, at):
        return pltpu.make_async_copy(src, dst, local.at[at])

    x_fetch = [fetch(x_hbm.at[b], x_all.at[b, pl.ds(0, nsig), strip(z), :], b) for b in range(nb)]
    p_fetch = [
        fetch(p_hbm.at[:, :, pl.ds(t * bs, bs)], p_all.at[me * bpd + t], nb + t) for t in range(bpd)
    ]
    pad_fetch = [fetch(x_hbm.at[b], xpad.at[b, pl.ds(0, nsig)], nb + bpd + b) for b in range(nb)]
    few_fetch = [
        fetch(src, dst, 2 * nb + bpd + at)
        for at, (src, dst) in enumerate(((sel_hbm, sel_ref), (pts_hbm, pts_ref), (w_hbm, w_ref)))
    ]
    for copy in x_fetch + p_fetch + pad_fetch + few_fetch:
        copy.start()
    pl.semaphore_wait(barrier, greeted)

    def remote(src, dst, send, recv, device):
        return pltpu.make_async_remote_copy(
            src_ref=src, dst_ref=dst, send_sem=send, recv_sem=recv, device_id=device, device_id_type=MESH
        )

    def x_copy(batch, h, owner, step):
        sems = x_up if step > 0 else x_down
        slot = x_all.at[batch, pl.ds(0, nsig), strip(owner), pl.ds(h * half, half)]
        return remote(slot, slot, sems, x_in.at[batch, h, owner], (me, z + step))

    def x_begin(batch, up, down):
        for h in range(HALVES):
            @pl.when(jnp.logical_and(z > 0, down))
            def _():
                x_copy(batch, h, z, -1).start()

            @pl.when(jnp.logical_and(z < nrows - 1, up))
            def _():
                x_copy(batch, h, z, 1).start()

    def x_next(batch, dist):
        if batch < nb:
            x_begin(batch, z == dist, nrows - 1 - z == dist)

    def x_forward(batch, dist):
        for h in range(HALVES):
            @pl.when(jnp.logical_and(z > 0, z + dist < nrows))
            def _():
                x_copy(batch, h, z + dist, -1).wait_recv()
                x_copy(batch, h, z + dist, -1).start()

            @pl.when(jnp.logical_and(z < nrows - 1, z - dist >= 0))
            def _():
                x_copy(batch, h, z - dist, 1).wait_recv()
                x_copy(batch, h, z - dist, 1).start()

    def x_wait(batch, h):
        for dist in range(1, nrows):
            @pl.when(z == 0)
            def _():
                x_copy(batch, h, dist, 1).wait_recv()

            @pl.when(z == nrows - 1)
            def _():
                x_copy(batch, h, nrows - 1 - dist, -1).wait_recv()

    def p_slot(owner, cut):
        span = nblk // pcuts
        return p_all.at[pl.ds(owner * bpd, bpd), pl.ds(cut * span, span)]

    def p_copy(owner, cut, k, to):
        return remote(p_slot(owner, cut), p_slot(owner, cut), p_out.at[k, cut], p_in.at[owner, cut], (peer(to), z))

    def p_forward(k, cut):
        owner = origin(k) if k else me
        return remote(p_slot(owner, cut), p_slot(owner, cut), p_pair.at[k, cut], p_in.at[owner, cut], (partner, z))

    def p_take(k, cut):
        p_copy(origin(k), cut, k, k).wait_recv()
        p_forward(k, cut).start()

    def p_relay(k, cut):
        return p_copy(origin(k), cut, 3, 3 - k)

    for copy in x_fetch:
        copy.wait()
    x_begin(0, True, True)
    x_next(1, 0)
    for copy in p_fetch:
        copy.wait()
    if square:
        for k, cut in ((1, 0), (2, 1), (1, 1), (2, 0)):
            p_copy(me, cut, k, k).start()
    else:
        for k in range(1, nchip):
            p_copy(me, 0, k, k).start()
    for cut in range(pcuts):
        p_forward(0, cut).start()

    for copy in pad_fetch + few_fetch:
        copy.wait()
    for batch in range(nb):
        x_all[batch, nsig] = jnp.zeros((bs, npts), BF16)
        xpad[batch, nsig] = jnp.zeros((rows, npts), BF16)
        pot[batch, nsig] = jnp.zeros((bs, npts), BF16)

        def invert(block, carry):
            found = jnp.int32(nsig)
            for s in range(nsig):
                found = jnp.where(sel_ref[batch, s] == block, jnp.int32(s), found)
            inv[batch, block] = found
            return carry
        lax.fori_loop(0, nblk, invert, 0)

        def fill(block, carry):
            lhs[pl.ds(pl.multiple_of(block * rows, rows), rows), batch * npts:(batch + 1) * npts] = xpad[
                batch, inv[batch, block]
            ]
            return carry
        lax.fori_loop(0, nblk, fill, 0)

    def fm_copy(batch, h, o):
        return remote(
            fm_send.at[batch, h, o], fm_all.at[batch, h, :, strip(z), :], fm_out,
            fm_in.at[batch, h], (me, middle + o),
        )

    def fm_wait(batch, h):
        others = fm_all.at[batch, h, :, pl.ds(0, bs - rows), :]
        remote(others, others, fm_out, fm_in.at[batch, h], (partner, z)).wait_recv()

    def choose(batch):
        def pick(s, carry):
            for t in range(nsig):
                psel[pl.ds(pl.multiple_of(s * rows, rows), rows), t * bs:(t + 1) * bs] = p_all[
                    sel_ref[batch, t], sel_ref[batch, s]
                ]
            return carry
        lax.fori_loop(0, nsig, pick, 0)

    def products(batch, h):
        got = jnp.dot(
            psel[...], x_all[batch, 0:nsig, :, h * half:(h + 1) * half].reshape(nsig * bs, half),
            preferred_element_type=F32,
        ).astype(BF16)
        for o in range(OWNERS):
            fm_send[batch, h, o] = got[:, o * quarter:(o + 1) * quarter].reshape(nsig, rows, quarter)
        for j in range(OWNERS):
            o = jnp.where(z <= middle, OWNERS - 1 - j, j)

            @pl.when(z != middle + o)
            def _():
                fm_copy(batch, h, o).start()
        for o in range(OWNERS):
            @pl.when(z == middle + o)
            def _():
                fm_all[batch, h, :, strip(z), :] = fm_send[batch, h, o]

    def m_copy(batch, h, o, step):
        sems = m_up if step > 0 else m_down
        piece = mixed.at[batch, h, pl.ds(o * quarter, quarter)]
        return remote(piece, piece, sems, m_in.at[batch, h, o], (me, z + step))

    def mix(batch, h, o):
        @pl.when(z == middle + o)
        def _():
            fm_wait(batch, h)
            at = h * half + o * quarter
            lanes = slice(at, at + quarter)
            flipped = jnp.concatenate(
                [pts_ref[axis, batch:batch + 1, lanes] for axis in range(3)] + [jnp.zeros((5, quarter), F32)], axis=0
            ).T
            inter = lax.dot_general(
                fm_all[batch, h].reshape(nsig * bs, quarter), x_all[batch, 0:nsig].reshape(nsig * bs, npts),
                (((0,), (0,)), ((), ())), preferred_element_type=F32,
            )
            dist2 = None
            for axis in range(3):
                diff = flipped[:, axis:axis + 1] - pts_ref[axis, batch:batch + 1, :]
                dist2 = diff * diff if dist2 is None else dist2 + diff * diff
            kern = 1.0 / jnp.sqrt(dist2 + 0.5)
            mixed[batch, h, o * quarter:(o + 1) * quarter, :] = (w_ref[batch:batch + 1, :] * kern * inter).astype(BF16)
            if middle + o > 0:
                m_copy(batch, h, o, -1).start()
            if middle + o < nrows - 1:
                m_copy(batch, h, o, 1).start()

    def m_pass(batch, h):
        for o in range(OWNERS):
            @pl.when(z < middle + o)
            def _():
                m_copy(batch, h, o, -1).wait_recv()

                @pl.when(z > 0)
                def _():
                    m_copy(batch, h, o, -1).start()

            @pl.when(z > middle + o)
            def _():
                m_copy(batch, h, o, 1).wait_recv()

                @pl.when(z < nrows - 1)
                def _():
                    m_copy(batch, h, o, 1).start()

    def potentials(batch, h):
        cut = slice(h * half, (h + 1) * half)

        def fill_pot(i, carry):
            some = pl.ds(i * 4, 4)
            got = lax.dot_general(
                x_all[batch, some].reshape(4 * bs, npts), mixed[batch, h], (((1,), (1,)), ((), ())),
                preferred_element_type=F32,
            ) * w_ref[batch:batch + 1, cut]
            pot[batch, some, :, cut] = got.astype(BF16).reshape(4, bs, half)
            return carry
        lax.fori_loop(0, nsig // 4, fill_pot, 0)

    x_forward(0, 1)
    x_next(1, 1)
    if square:
        for k, cut in ((1, 0), (2, 1)):
            p_take(k, cut)
            p_relay(k, cut).start()
    for dist in range(2, nrows - 1):
        x_forward(0, dist)
        x_next(1, dist)
    if square:
        for k, cut in ((1, 1), (2, 0)):
            p_take(k, cut)
        x_forward(1, 1)
        for cut in range(pcuts):
            p_take(3, cut)
    else:
        x_forward(1, 1)
        for k in range(1, nchip):
            p_take(k, 0)
    for k in range(nchip):
        for cut in range(pcuts):
            slot = source(k) * CORES + (CORES - 1 - core)
            remote(p_slot(slot, cut), p_slot(slot, cut), p_pair.at[k, cut], p_in.at[slot, cut], (partner, z)).wait_recv()
    choose(0)
    for h in range(HALVES):
        x_wait(0, h)
        products(0, h)
    for dist in range(2, nrows - 1):
        x_forward(1, dist)
    choose(1)
    for h in range(HALVES):
        x_wait(1, h)
        products(1, h)
    for h in range(HALVES):
        for o in range(OWNERS):
            mix(0, h, o)
    for h in range(HALVES):
        m_pass(0, h)
    total_rows = nblk * rows
    side = total_rows // 2
    step_rows = min(2 * GROUP, side)
    steps = total_rows // step_rows
    cut_steps = steps // 2
    groups = step_rows // GROUP
    early = (nb - 1) * npts

    def fill_rhs(dest):
        for t in range(bpd):
            for batch in range(nb):
                rhs[t * bs:(t + 1) * bs, batch * npts:(batch + 1) * npts] = pot[
                    batch, inv[batch, dest * bpd + t]
                ]

    def fill_early(dest):
        for t in range(bpd):
            for batch in range(nb - 1):
                rhs[t * bs:(t + 1) * bs, batch * npts:(batch + 1) * npts] = pot[batch, inv[batch, dest * bpd + t]]

    def fill_late(dest):
        batch = nb - 1
        some = [x_all[batch, inv[batch, dest * bpd + t]] for t in range(bpd)]
        got = lax.dot_general(
            some[0] if bpd == 1 else jnp.concatenate(some, axis=0), mixed[batch].reshape(npts, npts),
            (((1,), (1,)), ((), ())), preferred_element_type=F32,
        ) * w_ref[batch:batch + 1, :]
        rhs[:, early:nb * npts] = got.astype(BF16)

    def span(i):
        return pl.ds(pl.multiple_of(i * step_rows, step_rows), step_rows)

    def product(i, first=0, last=nb * npts):
        return lax.dot_general(
            lhs[span(i), first:last], rhs[:, first:last], (((1,), (1,)), ((), ())), preferred_element_type=F32
        )

    def pair_copy(k, i):
        came = far_in.at[i] if k == 3 and square else pair_in.at[k]
        return remote(pair_send.at[k, span(i)], pair_recv.at[k, span(i)], pair_out.at[k], came, (partner, z))

    def pair_whole(k):
        return remote(pair_send.at[k], pair_recv.at[k], pair_out.at[k], pair_in.at[k], (partner, z))

    def q_copy(k, i, device):
        return remote(q_send.at[k, span(i)], q_recv.at[k, span(i)], q_out.at[k - 1], q_in.at[k - 1, i], (device, z))

    def s_copy(k, i, device):
        return remote(s_send.at[k, i], s_recv.at[k, i], s_out.at[k - 1, i], s_in.at[k - 1, i], (device, z))

    def send(k, i, device):
        q_copy(k, i, device).start()
        s_copy(k, i, device).start()

    def arrive(k, i, device):
        q_copy(k, i, device).wait_recv()
        s_copy(k, i, device).wait_recv()

    def out_copy(i):
        return pltpu.make_async_copy(acc.at[span(i)], out_ref.at[span(i)], o_out.at[i])

    def encode(k, i, value):
        for g in range(groups):
            some = value[g * GROUP:(g + 1) * GROUP]
            top = jnp.maximum(jnp.max(jnp.abs(some), axis=0, keepdims=True), TINY)
            group = i * groups + g
            s_send[k, i, g:g + 1, :] = top * (1.0 / LEVELS)
            q_send[k, pl.ds(pl.multiple_of(group * GROUP, GROUP), GROUP), :] = (
                jnp.round(some * (LEVELS / top)).astype(jnp.int32).astype(jnp.int16)
            )

    def decode(k, i):
        parts = []
        for g in range(groups):
            group = i * groups + g
            at = pl.ds(pl.multiple_of(group * GROUP, GROUP), GROUP)
            parts.append(q_recv[k, at, :].astype(jnp.int32).astype(F32) * s_recv[k, i, g:g + 1, :])
        return parts[0] if groups == 1 else jnp.concatenate(parts, axis=0)

    def loop(first, last, step):
        def one(i, carry):
            step(i)
            return carry
        lax.fori_loop(first, last, one, 0)

    def theirs(k):
        fill_rhs(toward(k) * CORES + (CORES - 1 - core))

        def step(i):
            pair_send[k, span(i), :] = product(i)
            pair_copy(k, i).start()
        loop(0, steps, step)

    def ours(k, keeps):
        fill_rhs(toward(k) * CORES + core)
        pair_whole(k).wait_recv()
        for first, last, keep in keeps:
            def step(i):
                keep(k, i, product(i) + pair_recv[k, span(i), :])
            loop(first, last, step)

    def far_early():
        fill_early(toward(3) * CORES + (CORES - 1 - core))

        def step(i):
            pair_send[3, span(i), :] = product(i, 0, early)
        loop(0, steps, step)
        fill_early(toward(3) * CORES + core)

        def step(i):
            acc[span(i), :] = product(i, 0, early)
        loop(0, steps, step)

    def far_late(device):
        def weave(j):
            return lax.rem(j, 2) * cut_steps + j // 2

        fill_late(toward(3) * CORES + (CORES - 1 - core))

        def step(j):
            i = weave(j)
            pair_send[3, span(i), :] = pair_send[3, span(i), :] + product(i, early)
            pair_copy(3, i).start()
        loop(0, steps, step)
        fill_late(toward(3) * CORES + core)

        def step(j):
            i = weave(j)
            value = acc[span(i), :] + product(i, early)
            pair_copy(3, i).wait_recv()
            encode(3, i, value + pair_recv[3, span(i), :])
            send(3, i, device(i // cut_steps))
        loop(0, steps, step)

    def keep_code(device):
        def keep(k, i, value):
            encode(k, i, value)
            send(k, i, device)
        return keep

    def keep_value(k, i, value):
        pair_recv[k, span(i), :] = value

    def keep_out(k, i, value):
        acc[span(i), :] = value

    def add(k, first, last, device, final):
        def step(i):
            arrive(k, i, device)
            acc[span(i), :] = acc[span(i), :] + decode(k, i)
            if final:
                out_copy(i).start()
        loop(first, last, step)

    def drain_sums():
        for k in range(1, nchip):
            remote(q_send.at[k], q_recv.at[k], q_out.at[k - 1], q_in.at[k - 1, 0], (partner, z)).wait_send()
            loop(0, steps, lambda i: s_copy(k, i, partner).wait_send())

    def drain_early():
        for k in range(nchip):
            pair_whole(k).wait_send()
            for cut in range(pcuts):
                p_forward(k, cut).wait_send()
                if k > 0:
                    p_copy(me, cut, k, k).wait_send()

        def drain_one(cond, ref, sem):
            @pl.when(cond)
            def _():
                remote(ref, ref, sem, x_in.at[0, 0, 0], (partner, z)).wait_send()
        drain_one(jnp.logical_not(owns), fm_send, fm_out)
        drain_one(owns, fm_send.at[:, :, 0], fm_out)
        drain_one(z == middle, mixed.at[:, :, pl.ds(0, quarter)], m_up)
        drain_one(jnp.logical_and(z > middle, z < nrows - 1), mixed, m_up)
        drain_one(z == middle + 1, mixed.at[:, :, pl.ds(0, quarter)], m_down)
        drain_one(jnp.logical_and(z <= middle, z > 0), mixed, m_down)
        for at in range(nrows):
            if at < nrows - 1:
                drain_one(z == at, x_all.at[:, pl.ds(0, nsig), pl.ds(0, (at + 1) * rows)], x_up)
            if at > 0:
                drain_one(z == at, x_all.at[:, pl.ds(0, nsig), pl.ds(0, (nrows - at) * rows)], x_down)

    low, high = (0, cut_steps), (cut_steps, steps)
    @pl.when(owns)
    def _():
        for h in range(HALVES):
            for o in range(OWNERS):
                mix(1, h, o)
            if h == 0:
                for other in range(HALVES):
                    potentials(0, other)
        for h in range(HALVES):
            if h == HALVES - 1 and square:
                far_early()
            m_pass(1, h)
        if not square:
            for h in range(HALVES - 1):
                potentials(1, h)

    @pl.when(jnp.logical_not(owns))
    def _():
        for h in range(HALVES):
            potentials(0, h)
        if square:
            far_early()
        for h in range(HALVES):
            m_pass(1, h)
        if not square:
            for h in range(HALVES - 1):
                potentials(1, h)

    if square:
        flip = {1: peer(1), 2: peer(2)}
        far_late(lambda cut: flip[1] + cut * (flip[2] - flip[1]))
        for h in range(HALVES):
            potentials(1, h)
        theirs(1)
        theirs(2)
        ours(1, [(*low, keep_code(flip[1])), (*high, keep_value)])
        theirs(0)
        ours(2, [(*high, keep_code(flip[2])), (*low, keep_value)])
        ours(0, [(0, steps, keep_out)])
        for k, cut in ((1, high), (2, low)):
            def relay(i):
                arrive(3, i, flip[3 - k])
                encode(k, i, pair_recv[k, span(i), :] + decode(3, i))
                send(k, i, flip[k])
            loop(*cut, relay)
        add(1, *low, flip[1], False)
        add(2, *high, flip[2], False)
        drain_early()
        add(1, *high, flip[1], True)
        add(2, *low, flip[2], True)
        drain_sums()
    else:
        potentials(1, HALVES - 1)
        for k in range(1, nchip):
            theirs(k)
            ours(k, [(0, steps, keep_code(peer(k)))])
        theirs(0)
        ours(0, [(0, steps, keep_out)])
        for k in range(1, nchip):
            add(k, 0, steps, peer(k), k == nchip - 1)
        drain_sums()
        drain_early()

    def drain_out(i):
        out_copy(i).wait()
    loop(0, steps, drain_out)


def deliver(sum_ref, out_ref, buf, came, went):
    span = sum_ref.shape[0] // CHUNKS
    cuts = [pl.ds(i * span, span) for i in range(CHUNKS)]
    ins = [pltpu.make_async_copy(sum_ref.at[cut], buf.at[cut], came.at[i]) for i, cut in enumerate(cuts)]
    outs = [pltpu.make_async_copy(buf.at[cut], out_ref.at[cut], went.at[i]) for i, cut in enumerate(cuts)]
    for copy in ins:
        copy.start()
    for copy_in, copy_out in zip(ins, outs):
        copy_in.wait()
        copy_out.start()
    for copy in outs:
        copy.wait()


def body(ngrid, nrows, density, basis_values, grid_points, grid_weights, screened_blocks):
    nblk, rows, cols = density.shape
    nb, nsig, _, npts = basis_values.shape
    bs = rows * nrows
    nchip = ngrid // CORES
    half = npts // HALVES
    quarter = half // OWNERS
    total_rows = nblk * rows
    step_rows = min(2 * GROUP, total_rows // 2)
    steps = total_rows // step_rows
    anywhere = pl.BlockSpec(memory_space=pl.ANY)
    dma = pltpu.SemaphoreType.DMA
    out = pl.pallas_call(
        functools.partial(kernel, ngrid, nrows),
        out_shape=jax.ShapeDtypeStruct((total_rows, cols), F32),
        in_specs=[anywhere] * 5,
        out_specs=anywhere,
        scratch_shapes=[
            pltpu.SMEM((nb, nsig), jnp.int32),
            pltpu.VMEM((3, nb, npts), F32),
            pltpu.VMEM((nb, npts), F32),
            pltpu.SMEM((nb, nblk), jnp.int32),
            pltpu.VMEM((nblk, nblk, rows, bs), BF16),
            pltpu.VMEM((nb, nsig + 1, bs, npts), BF16),
            pltpu.VMEM((nsig * rows, nsig * bs), BF16),
            pltpu.VMEM((nb, HALVES, OWNERS, nsig, rows, quarter), BF16),
            pltpu.VMEM((nb, HALVES, nsig, bs, quarter), BF16),
            pltpu.VMEM((nb, HALVES, half, npts), BF16),
            pltpu.VMEM((nb, nsig + 1, rows, npts), BF16),
            pltpu.VMEM((nb, nsig + 1, bs, npts), BF16),
            pltpu.VMEM((total_rows, nb * npts), BF16),
            pltpu.VMEM((cols, nb * npts), BF16),
            pltpu.VMEM((total_rows, cols), F32),
            pltpu.VMEM((nchip, total_rows, cols), F32),
            pltpu.VMEM((nchip, total_rows, cols), F32),
            pltpu.VMEM((nchip, total_rows, cols), jnp.int16),
            pltpu.VMEM((nchip, total_rows, cols), jnp.int16),
            pltpu.VMEM((nchip, steps, step_rows // GROUP, cols), F32),
            pltpu.VMEM((nchip, steps, step_rows // GROUP, cols), F32),
            dma((nchip, 2)), dma((nchip, 2)), dma((ngrid, 2)),
            dma(()), dma(()), dma((nb, HALVES, nrows)),
            dma(()), dma((nb, HALVES)),
            dma(()), dma(()), dma((nb, HALVES, OWNERS)),
            dma((nchip,)), dma((nchip,)), dma((steps,)),
            dma((nchip - 1,)), dma((nchip - 1, steps)), dma((nchip - 1, steps)), dma((nchip - 1, steps)),
            dma((steps,)), dma((2 * nb + cols // bs + 3,)),
        ],
        compiler_params=pltpu.CompilerParams(
            collective_id=0, has_side_effects=True, vmem_limit_bytes=63 * 1024 * 1024
        ),
        name="exchange",
    )(screened_blocks, density, basis_values, jnp.transpose(grid_points, (1, 0, 2)), grid_weights)
    out = pl.pallas_call(
        deliver,
        out_shape=jax.ShapeDtypeStruct((total_rows, cols), F32),
        in_specs=[anywhere],
        out_specs=anywhere,
        scratch_shapes=[pltpu.VMEM((total_rows, cols), F32), dma((CHUNKS,)), dma((CHUNKS,))],
        name="deliver",
    )(out)
    return out.reshape(nblk, rows, cols)


def solution(mesh):
    placed = (
        P(None, "rows", "grid"),
        P("grid", None, "rows", None),
        P("grid", None, None),
        P("grid", None),
        P("grid", None),
    )
    return jax.shard_map(
        functools.partial(body, mesh.shape["grid"], mesh.shape["rows"]), mesh=mesh, in_specs=placed,
        out_specs=P(None, "rows", "grid"), check_vma=False,
    )
```

```python
import functools

import jax
import jax.numpy as jnp
from jax import lax
from jax.experimental import pallas as pl
from jax.experimental.pallas import tpu as pltpu
from jax.sharding import PartitionSpec as P

MESH = pl.DeviceIdType.MESH
F32 = jnp.float32
BF16 = jnp.bfloat16
CORES = 2
GROUP = 128
HALVES = 2
OWNERS = 2
CHUNKS = 8
LEVELS = 32767.0
TINY = 2.0 ** -110


def kernel(
    ngrid, nrows, sel_hbm, p_hbm, x_hbm, pts_hbm, w_hbm, out_ref,
    sel_ref, pts_ref, w_ref, inv, p_all, x_all, psel, fm_send, fm_all, mixed, xpad, pot, lhs, rhs, acc, pair_send, pair_recv,
    q_send, q_recv, s_send, s_recv,
    p_out, p_pair, p_in, x_up, x_down, x_in, fm_out, fm_in, m_up, m_down, m_in,
    pair_out, pair_in, q_out, q_in, s_out, s_in, o_out, local,
):
    me = lax.axis_index("grid")
    z = lax.axis_index("rows")
    core = lax.rem(me, CORES)
    chip = me // CORES
    nchip = ngrid // CORES
    square = nchip == 4
    partner = chip * CORES + (CORES - 1 - core)
    nblk, rows, cols = p_hbm.shape
    nb, nsig, _, npts = x_hbm.shape
    bs = rows * nrows
    bpd = cols // bs
    half = npts // HALVES
    quarter = half // OWNERS
    middle = nrows // 2 - 1
    owns = jnp.logical_and(z >= middle, z < middle + OWNERS)
    pcuts = 2 if square else 1

    def toward(k):
        if square:
            return chip + (k % 2) * (1 - 2 * lax.rem(chip, 2)) + (k // 2) * (2 - 4 * (chip // 2))
        return lax.rem(chip + k, nchip)

    def source(k):
        return toward(k) if square else lax.rem(chip + nchip - k, nchip)

    def peer(k):
        return toward(k) * CORES + core

    def origin(k):
        return source(k) * CORES + core

    barrier = pltpu.get_barrier_semaphore()
    greeted = jnp.int32(1)
    for other in range(nrows):
        near = jnp.logical_or(other == z + 1, other == z - 1)
        if middle <= other < middle + OWNERS:
            near = other != z
        else:
            near = jnp.logical_or(near, jnp.logical_and(owns, other != z))
        greeted = greeted + near.astype(jnp.int32)

        @pl.when(near)
        def _():
            pl.semaphore_signal(barrier, inc=1, device_id=(me, other), device_id_type=MESH)
    for k in (1, 2) if square else range(1, nchip):
        greeted = greeted + 1
        pl.semaphore_signal(barrier, inc=1, device_id=(peer(k), z), device_id_type=MESH)
    pl.semaphore_signal(barrier, inc=1, device_id=(partner, z), device_id_type=MESH)

    def strip(owner):
        return pl.ds(pl.multiple_of(owner * rows, rows), rows)

    def fetch(src, dst, at):
        return pltpu.make_async_copy(src, dst, local.at[at])

    x_fetch = [fetch(x_hbm.at[b], x_all.at[b, pl.ds(0, nsig), strip(z), :], b) for b in range(nb)]
    p_fetch = [
        fetch(p_hbm.at[:, :, pl.ds(t * bs, bs)], p_all.at[me * bpd + t], nb + t) for t in range(bpd)
    ]
    pad_fetch = [fetch(x_hbm.at[b], xpad.at[b, pl.ds(0, nsig)], nb + bpd + b) for b in range(nb)]
    few_fetch = [
        fetch(src, dst, 2 * nb + bpd + at)
        for at, (src, dst) in enumerate(((sel_hbm, sel_ref), (pts_hbm, pts_ref), (w_hbm, w_ref)))
    ]
    for copy in x_fetch + p_fetch + pad_fetch + few_fetch:
        copy.start()
    pl.semaphore_wait(barrier, greeted)

    def remote(src, dst, send, recv, device):
        return pltpu.make_async_remote_copy(
            src_ref=src, dst_ref=dst, send_sem=send, recv_sem=recv, device_id=device, device_id_type=MESH
        )

    def x_copy(batch, h, owner, step):
        sems = x_up if step > 0 else x_down
        slot = x_all.at[batch, pl.ds(0, nsig), strip(owner), pl.ds(h * half, half)]
        return remote(slot, slot, sems, x_in.at[batch, h, owner], (me, z + step))

    def x_begin(batch, up, down):
        for h in range(HALVES):
            @pl.when(jnp.logical_and(z > 0, down))
            def _():
                x_copy(batch, h, z, -1).start()

            @pl.when(jnp.logical_and(z < nrows - 1, up))
            def _():
                x_copy(batch, h, z, 1).start()

    def x_next(batch, dist):
        if batch < nb:
            x_begin(batch, z == dist, nrows - 1 - z == dist)

    def x_forward(batch, dist):
        for h in range(HALVES):
            @pl.when(jnp.logical_and(z > 0, z + dist < nrows))
            def _():
                x_copy(batch, h, z + dist, -1).wait_recv()
                x_copy(batch, h, z + dist, -1).start()

            @pl.when(jnp.logical_and(z < nrows - 1, z - dist >= 0))
            def _():
                x_copy(batch, h, z - dist, 1).wait_recv()
                x_copy(batch, h, z - dist, 1).start()

    def x_wait(batch, h):
        for dist in range(1, nrows):
            @pl.when(z == 0)
            def _():
                x_copy(batch, h, dist, 1).wait_recv()

            @pl.when(z == nrows - 1)
            def _():
                x_copy(batch, h, nrows - 1 - dist, -1).wait_recv()

    def p_slot(owner, cut):
        span = nblk // pcuts
        return p_all.at[pl.ds(owner * bpd, bpd), pl.ds(cut * span, span)]

    def p_copy(owner, cut, k, to):
        return remote(p_slot(owner, cut), p_slot(owner, cut), p_out.at[k, cut], p_in.at[owner, cut], (peer(to), z))

    def p_forward(k, cut):
        owner = origin(k) if k else me
        return remote(p_slot(owner, cut), p_slot(owner, cut), p_pair.at[k, cut], p_in.at[owner, cut], (partner, z))

    def p_take(k, cut):
        p_copy(origin(k), cut, k, k).wait_recv()
        p_forward(k, cut).start()

    def p_relay(k, cut):
        return p_copy(origin(k), cut, 3, 3 - k)

    for copy in x_fetch:
        copy.wait()
    x_begin(0, True, True)
    x_next(1, 0)
    for copy in p_fetch:
        copy.wait()
    if square:
        for k, cut in ((1, 0), (2, 1), (1, 1), (2, 0)):
            p_copy(me, cut, k, k).start()
    else:
        for k in range(1, nchip):
            p_copy(me, 0, k, k).start()
    for cut in range(pcuts):
        p_forward(0, cut).start()

    for copy in pad_fetch + few_fetch:
        copy.wait()
    for batch in range(nb):
        x_all[batch, nsig] = jnp.zeros((bs, npts), BF16)
        xpad[batch, nsig] = jnp.zeros((rows, npts), BF16)
        pot[batch, nsig] = jnp.zeros((bs, npts), BF16)

        def invert(block, carry):
            found = jnp.int32(nsig)
            for s in range(nsig):
                found = jnp.where(sel_ref[batch, s] == block, jnp.int32(s), found)
            inv[batch, block] = found
            return carry
        lax.fori_loop(0, nblk, invert, 0)

        def fill(block, carry):
            lhs[pl.ds(pl.multiple_of(block * rows, rows), rows), batch * npts:(batch + 1) * npts] = xpad[
                batch, inv[batch, block]
            ]
            return carry
        lax.fori_loop(0, nblk, fill, 0)

    def fm_copy(batch, h, o):
        return remote(
            fm_send.at[batch, h, o], fm_all.at[batch, h, :, strip(z), :], fm_out,
            fm_in.at[batch, h], (me, middle + o),
        )

    def fm_wait(batch, h):
        others = fm_all.at[batch, h, :, pl.ds(0, bs - rows), :]
        remote(others, others, fm_out, fm_in.at[batch, h], (partner, z)).wait_recv()

    def choose(batch):
        def pick(s, carry):
            for t in range(nsig):
                psel[pl.ds(pl.multiple_of(s * rows, rows), rows), t * bs:(t + 1) * bs] = p_all[
                    sel_ref[batch, t], sel_ref[batch, s]
                ]
            return carry
        lax.fori_loop(0, nsig, pick, 0)

    def products(batch, h):
        got = jnp.dot(
            psel[...], x_all[batch, 0:nsig, :, h * half:(h + 1) * half].reshape(nsig * bs, half),
            preferred_element_type=F32,
        ).astype(BF16)
        for o in range(OWNERS):
            fm_send[batch, h, o] = got[:, o * quarter:(o + 1) * quarter].reshape(nsig, rows, quarter)
        for j in range(OWNERS):
            o = jnp.where(z <= middle, OWNERS - 1 - j, j)

            @pl.when(z != middle + o)
            def _():
                fm_copy(batch, h, o).start()
        for o in range(OWNERS):
            @pl.when(z == middle + o)
            def _():
                fm_all[batch, h, :, strip(z), :] = fm_send[batch, h, o]

    def m_copy(batch, h, o, step):
        sems = m_up if step > 0 else m_down
        piece = mixed.at[batch, h, pl.ds(o * quarter, quarter)]
        return remote(piece, piece, sems, m_in.at[batch, h, o], (me, z + step))

    def mix(batch, h, o):
        @pl.when(z == middle + o)
        def _():
            fm_wait(batch, h)
            at = h * half + o * quarter
            lanes = slice(at, at + quarter)
            flipped = jnp.concatenate(
                [pts_ref[axis, batch:batch + 1, lanes] for axis in range(3)] + [jnp.zeros((5, quarter), F32)], axis=0
            ).T
            inter = lax.dot_general(
                fm_all[batch, h].reshape(nsig * bs, quarter), x_all[batch, 0:nsig].reshape(nsig * bs, npts),
                (((0,), (0,)), ((), ())), preferred_element_type=F32,
            )
            dist2 = None
            for axis in range(3):
                diff = flipped[:, axis:axis + 1] - pts_ref[axis, batch:batch + 1, :]
                dist2 = diff * diff if dist2 is None else dist2 + diff * diff
            kern = 1.0 / jnp.sqrt(dist2 + 0.5)
            mixed[batch, h, o * quarter:(o + 1) * quarter, :] = (w_ref[batch:batch + 1, :] * kern * inter).astype(BF16)
            if middle + o > 0:
                m_copy(batch, h, o, -1).start()
            if middle + o < nrows - 1:
                m_copy(batch, h, o, 1).start()

    def m_pass(batch, h):
        for o in range(OWNERS):
            @pl.when(z < middle + o)
            def _():
                m_copy(batch, h, o, -1).wait_recv()

                @pl.when(z > 0)
                def _():
                    m_copy(batch, h, o, -1).start()

            @pl.when(z > middle + o)
            def _():
                m_copy(batch, h, o, 1).wait_recv()

                @pl.when(z < nrows - 1)
                def _():
                    m_copy(batch, h, o, 1).start()

    def potentials(batch, h):
        cut = slice(h * half, (h + 1) * half)

        def fill_pot(i, carry):
            some = pl.ds(i * 4, 4)
            got = lax.dot_general(
                x_all[batch, some].reshape(4 * bs, npts), mixed[batch, h], (((1,), (1,)), ((), ())),
                preferred_element_type=F32,
            ) * w_ref[batch:batch + 1, cut]
            pot[batch, some, :, cut] = got.astype(BF16).reshape(4, bs, half)
            return carry
        lax.fori_loop(0, nsig // 4, fill_pot, 0)

    x_forward(0, 1)
    x_next(1, 1)
    if square:
        for k, cut in ((1, 0), (2, 1)):
            p_take(k, cut)
            p_relay(k, cut).start()
    for dist in range(2, nrows - 1):
        x_forward(0, dist)
        x_next(1, dist)
    if square:
        for k, cut in ((1, 1), (2, 0)):
            p_take(k, cut)
        x_forward(1, 1)
        for cut in range(pcuts):
            p_take(3, cut)
    else:
        x_forward(1, 1)
        for k in range(1, nchip):
            p_take(k, 0)
    for k in range(nchip):
        for cut in range(pcuts):
            slot = source(k) * CORES + (CORES - 1 - core)
            remote(p_slot(slot, cut), p_slot(slot, cut), p_pair.at[k, cut], p_in.at[slot, cut], (partner, z)).wait_recv()
    choose(0)
    for h in range(HALVES):
        x_wait(0, h)
        products(0, h)
    for dist in range(2, nrows - 1):
        x_forward(1, dist)
    choose(1)
    for h in range(HALVES):
        x_wait(1, h)
        products(1, h)
    for h in range(HALVES):
        for o in range(OWNERS):
            mix(0, h, o)
    for h in range(HALVES):
        m_pass(0, h)
    total_rows = nblk * rows
    side = total_rows // 2
    step_rows = min(2 * GROUP, side)
    steps = total_rows // step_rows
    cut_steps = steps // 2
    groups = step_rows // GROUP
    early = (nb - 1) * npts

    def fill_rhs(dest):
        for t in range(bpd):
            for batch in range(nb):
                rhs[t * bs:(t + 1) * bs, batch * npts:(batch + 1) * npts] = pot[
                    batch, inv[batch, dest * bpd + t]
                ]

    def fill_early(dest):
        for t in range(bpd):
            for batch in range(nb - 1):
                rhs[t * bs:(t + 1) * bs, batch * npts:(batch + 1) * npts] = pot[batch, inv[batch, dest * bpd + t]]

    def fill_late(dest):
        batch, known = nb - 1, npts - half
        some = []
        for t in range(bpd):
            slot = inv[batch, dest * bpd + t]
            rhs[t * bs:(t + 1) * bs, early:early + known] = pot[batch, slot, :, 0:known]
            some.append(x_all[batch, slot])
        got = lax.dot_general(
            some[0] if bpd == 1 else jnp.concatenate(some, axis=0), mixed[batch, HALVES - 1],
            (((1,), (1,)), ((), ())), preferred_element_type=F32,
        ) * w_ref[batch:batch + 1, known:npts]
        rhs[:, early + known:nb * npts] = got.astype(BF16)

    def span(i):
        return pl.ds(pl.multiple_of(i * step_rows, step_rows), step_rows)

    def product(i, first=0, last=nb * npts):
        return lax.dot_general(
            lhs[span(i), first:last], rhs[:, first:last], (((1,), (1,)), ((), ())), preferred_element_type=F32
        )

    def pair_copy(k, i):
        return remote(
            pair_send.at[k, span(i)], pair_recv.at[k, span(i)], pair_out.at[k], pair_in.at[k, i], (partner, z)
        )

    def q_copy(k, i, device):
        return remote(q_send.at[k, span(i)], q_recv.at[k, span(i)], q_out.at[k - 1], q_in.at[k - 1, i], (device, z))

    def s_copy(k, i, device):
        return remote(s_send.at[k, i], s_recv.at[k, i], s_out.at[k - 1, i], s_in.at[k - 1, i], (device, z))

    def send(k, i, device):
        q_copy(k, i, device).start()
        s_copy(k, i, device).start()

    def arrive(k, i, device):
        q_copy(k, i, device).wait_recv()
        s_copy(k, i, device).wait_recv()

    def out_copy(i):
        return pltpu.make_async_copy(acc.at[span(i)], out_ref.at[span(i)], o_out.at[i])

    def encode(k, i, value):
        for g in range(groups):
            some = value[g * GROUP:(g + 1) * GROUP]
            top = jnp.maximum(jnp.max(jnp.abs(some), axis=0, keepdims=True), TINY)
            group = i * groups + g
            s_send[k, i, g:g + 1, :] = top * (1.0 / LEVELS)
            q_send[k, pl.ds(pl.multiple_of(group * GROUP, GROUP), GROUP), :] = (
                jnp.round(some * (LEVELS / top)).astype(jnp.int32).astype(jnp.int16)
            )

    def decode(k, i):
        parts = []
        for g in range(groups):
            group = i * groups + g
            at = pl.ds(pl.multiple_of(group * GROUP, GROUP), GROUP)
            parts.append(q_recv[k, at, :].astype(jnp.int32).astype(F32) * s_recv[k, i, g:g + 1, :])
        return parts[0] if groups == 1 else jnp.concatenate(parts, axis=0)

    def loop(first, last, step):
        def one(i, carry):
            step(i)
            return carry
        lax.fori_loop(first, last, one, 0)

    def theirs(k):
        fill_rhs(toward(k) * CORES + (CORES - 1 - core))

        def step(i):
            pair_send[k, span(i), :] = product(i)
            pair_copy(k, i).start()
        loop(0, steps, step)

    def ours(k, keeps):
        fill_rhs(toward(k) * CORES + core)
        for first, last, keep in keeps:
            def step(i):
                pair_copy(k, i).wait_recv()
                keep(k, i, product(i) + pair_recv[k, span(i), :])
            loop(first, last, step)

    def far_early():
        fill_early(toward(3) * CORES + (CORES - 1 - core))

        def step(i):
            pair_send[3, span(i), :] = product(i, 0, early)
        loop(0, steps, step)
        fill_early(toward(3) * CORES + core)

        def step(i):
            acc[span(i), :] = product(i, 0, early)
        loop(0, steps, step)

    def far_late(device):
        def weave(j):
            return lax.rem(j, 2) * cut_steps + j // 2

        fill_late(toward(3) * CORES + (CORES - 1 - core))

        def step(j):
            i = weave(j)
            pair_send[3, span(i), :] = pair_send[3, span(i), :] + product(i, early)
            pair_copy(3, i).start()
        loop(0, steps, step)
        fill_late(toward(3) * CORES + core)

        def step(j):
            i = weave(j)
            value = acc[span(i), :] + product(i, early)
            pair_copy(3, i).wait_recv()
            encode(3, i, value + pair_recv[3, span(i), :])
            send(3, i, device(i // cut_steps))
        loop(0, steps, step)

    def keep_code(device):
        def keep(k, i, value):
            encode(k, i, value)
            send(k, i, device)
        return keep

    def keep_value(k, i, value):
        pair_recv[k, span(i), :] = value

    def keep_out(k, i, value):
        acc[span(i), :] = value

    def add(k, first, last, device, final):
        def step(i):
            arrive(k, i, device)
            acc[span(i), :] = acc[span(i), :] + decode(k, i)
            if final:
                out_copy(i).start()
        loop(first, last, step)

    def drain_sums():
        for k in range(1, nchip):
            remote(q_send.at[k], q_recv.at[k], q_out.at[k - 1], q_in.at[k - 1, 0], (partner, z)).wait_send()
            loop(0, steps, lambda i: s_copy(k, i, partner).wait_send())

    def drain_early():
        for k in range(nchip):
            remote(pair_send.at[k], pair_recv.at[k], pair_out.at[k], pair_in.at[k, 0], (partner, z)).wait_send()
            for cut in range(pcuts):
                p_forward(k, cut).wait_send()
                if k > 0:
                    p_copy(me, cut, k, k).wait_send()

        def drain_one(cond, ref, sem):
            @pl.when(cond)
            def _():
                remote(ref, ref, sem, x_in.at[0, 0, 0], (partner, z)).wait_send()
        drain_one(jnp.logical_not(owns), fm_send, fm_out)
        drain_one(owns, fm_send.at[:, :, 0], fm_out)
        drain_one(z == middle, mixed.at[:, :, pl.ds(0, quarter)], m_up)
        drain_one(jnp.logical_and(z > middle, z < nrows - 1), mixed, m_up)
        drain_one(z == middle + 1, mixed.at[:, :, pl.ds(0, quarter)], m_down)
        drain_one(jnp.logical_and(z <= middle, z > 0), mixed, m_down)
        for at in range(nrows):
            if at < nrows - 1:
                drain_one(z == at, x_all.at[:, pl.ds(0, nsig), pl.ds(0, (at + 1) * rows)], x_up)
            if at > 0:
                drain_one(z == at, x_all.at[:, pl.ds(0, nsig), pl.ds(0, (nrows - at) * rows)], x_down)

    low, high = (0, cut_steps), (cut_steps, steps)
    @pl.when(owns)
    def _():
        for h in range(HALVES):
            for o in range(OWNERS):
                mix(1, h, o)
            if h == 0:
                for other in range(HALVES):
                    potentials(0, other)
        for h in range(HALVES):
            if h == HALVES - 1 and square:
                far_early()
            m_pass(1, h)
        for h in range(HALVES - 1):
            potentials(1, h)

    @pl.when(jnp.logical_not(owns))
    def _():
        for h in range(HALVES):
            potentials(0, h)
        if square:
            far_early()
        for h in range(HALVES):
            m_pass(1, h)
            if h < HALVES - 1:
                potentials(1, h)

    if square:
        flip = {1: peer(1), 2: peer(2)}
        far_late(lambda cut: flip[1] + cut * (flip[2] - flip[1]))
        potentials(1, HALVES - 1)
        theirs(1)
        theirs(2)
        ours(1, [(*low, keep_code(flip[1])), (*high, keep_value)])
        ours(2, [(*high, keep_code(flip[2])), (*low, keep_value)])
        theirs(0)
        ours(0, [(0, steps, keep_out)])
        for k, cut in ((1, high), (2, low)):
            def relay(i):
                arrive(3, i, flip[3 - k])
                encode(k, i, pair_recv[k, span(i), :] + decode(3, i))
                send(k, i, flip[k])
            loop(*cut, relay)
        add(1, *low, flip[1], False)
        add(2, *high, flip[2], False)
        drain_early()
        add(1, *high, flip[1], True)
        add(2, *low, flip[2], True)
        drain_sums()
    else:
        potentials(1, HALVES - 1)
        for k in range(1, nchip):
            theirs(k)
            ours(k, [(0, steps, keep_code(peer(k)))])
        theirs(0)
        ours(0, [(0, steps, keep_out)])
        for k in range(1, nchip):
            add(k, 0, steps, peer(k), k == nchip - 1)
        drain_sums()
        drain_early()

    def drain_out(i):
        out_copy(i).wait()
    loop(0, steps, drain_out)


def deliver(sum_ref, out_ref, buf, came, went):
    span = sum_ref.shape[0] // CHUNKS
    cuts = [pl.ds(i * span, span) for i in range(CHUNKS)]
    ins = [pltpu.make_async_copy(sum_ref.at[cut], buf.at[cut], came.at[i]) for i, cut in enumerate(cuts)]
    outs = [pltpu.make_async_copy(buf.at[cut], out_ref.at[cut], went.at[i]) for i, cut in enumerate(cuts)]
    for copy in ins:
        copy.start()
    for copy_in, copy_out in zip(ins, outs):
        copy_in.wait()
        copy_out.start()
    for copy in outs:
        copy.wait()


def body(ngrid, nrows, density, basis_values, grid_points, grid_weights, screened_blocks):
    nblk, rows, cols = density.shape
    nb, nsig, _, npts = basis_values.shape
    bs = rows * nrows
    nchip = ngrid // CORES
    half = npts // HALVES
    quarter = half // OWNERS
    total_rows = nblk * rows
    step_rows = min(2 * GROUP, total_rows // 2)
    steps = total_rows // step_rows
    anywhere = pl.BlockSpec(memory_space=pl.ANY)
    dma = pltpu.SemaphoreType.DMA
    out = pl.pallas_call(
        functools.partial(kernel, ngrid, nrows),
        out_shape=jax.ShapeDtypeStruct((total_rows, cols), F32),
        in_specs=[anywhere] * 5,
        out_specs=anywhere,
        scratch_shapes=[
            pltpu.SMEM((nb, nsig), jnp.int32),
            pltpu.VMEM((3, nb, npts), F32),
            pltpu.VMEM((nb, npts), F32),
            pltpu.SMEM((nb, nblk), jnp.int32),
            pltpu.VMEM((nblk, nblk, rows, bs), BF16),
            pltpu.VMEM((nb, nsig + 1, bs, npts), BF16),
            pltpu.VMEM((nsig * rows, nsig * bs), BF16),
            pltpu.VMEM((nb, HALVES, OWNERS, nsig, rows, quarter), BF16),
            pltpu.VMEM((nb, HALVES, nsig, bs, quarter), BF16),
            pltpu.VMEM((nb, HALVES, half, npts), BF16),
            pltpu.VMEM((nb, nsig + 1, rows, npts), BF16),
            pltpu.VMEM((nb, nsig + 1, bs, npts), BF16),
            pltpu.VMEM((total_rows, nb * npts), BF16),
            pltpu.VMEM((cols, nb * npts), BF16),
            pltpu.VMEM((total_rows, cols), F32),
            pltpu.VMEM((nchip, total_rows, cols), F32),
            pltpu.VMEM((nchip, total_rows, cols), F32),
            pltpu.VMEM((nchip, total_rows, cols), jnp.int16),
            pltpu.VMEM((nchip, total_rows, cols), jnp.int16),
            pltpu.VMEM((nchip, steps, step_rows // GROUP, cols), F32),
            pltpu.VMEM((nchip, steps, step_rows // GROUP, cols), F32),
            dma((nchip, 2)), dma((nchip, 2)), dma((ngrid, 2)),
            dma(()), dma(()), dma((nb, HALVES, nrows)),
            dma(()), dma((nb, HALVES)),
            dma(()), dma(()), dma((nb, HALVES, OWNERS)),
            dma((nchip,)), dma((nchip, steps)),
            dma((nchip - 1,)), dma((nchip - 1, steps)), dma((nchip - 1, steps)), dma((nchip - 1, steps)),
            dma((steps,)), dma((2 * nb + cols // bs + 3,)),
        ],
        compiler_params=pltpu.CompilerParams(
            collective_id=0, has_side_effects=True, vmem_limit_bytes=63 * 1024 * 1024
        ),
        name="exchange",
    )(screened_blocks, density, basis_values, jnp.transpose(grid_points, (1, 0, 2)), grid_weights)
    out = pl.pallas_call(
        deliver,
        out_shape=jax.ShapeDtypeStruct((total_rows, cols), F32),
        in_specs=[anywhere],
        out_specs=anywhere,
        scratch_shapes=[pltpu.VMEM((total_rows, cols), F32), dma((CHUNKS,)), dma((CHUNKS,))],
        name="deliver",
    )(out)
    return out.reshape(nblk, rows, cols)


def solution(mesh):
    placed = (
        P(None, "rows", "grid"),
        P("grid", None, "rows", None),
        P("grid", None, None),
        P("grid", None),
        P("grid", None),
    )
    return jax.shard_map(
        functools.partial(body, mesh.shape["grid"], mesh.shape["rows"]), mesh=mesh, in_specs=placed,
        out_specs=P(None, "rows", "grid"), check_vma=False,
    )
```
